128 devices in a mesh: rep: 1, tp: 16 (over z, y), dp: 8 (over x, core).
Axes of the slice: x: 4, y: 4, z: 4, core: 2. Of those that a mesh axis runs over, the one named last changes fastest.
Arguments:
- grad_partial: float32 [8, 8, 1024, 2048], P(('rep', 'dp'), None, None, 'tp')
- momentum: float32 [8, 1024, 2048], P('rep', 'dp', 'tp')
- weight: float32 [8, 1024, 2048], P('rep', 'dp', 'tp')
- learn_rate: float32 [8], P('rep')
- decay_rate: float32 [], replicated
Outputs:
- output 1: float32 [8, 1024, 2048], P('rep', 'dp', 'tp')
- output 2: float32 [8, 1024, 2048], P('rep', 'dp', 'tp')
- output 3: bfloat16 [8, 1024, 2048], P('rep', None, 'tp')
All inputs are finite; a program needn't handle non-finite values.
Results may differ from the reference program's by a relative error of at most 0.0131549.
Values are sent between devices in bfloat16 or wider.
A program may use at most 1 GiB of HBM per device.

```python
import math
import jax
import jax.numpy as jnp
from jax import lax

DP_SIZE = 8
MATS = 8
ROWS = 1024
COLS = 2048

MOMENTUM = 0.95
NS_STEPS = 5
COEF_A = 3.4445
COEF_B = -4.7750
COEF_C = 2.0315
NORM_EPS = 1e-7
OUT_SCALE = 0.2 * math.sqrt(max(ROWS, COLS))


def setup_inputs(seed: int = 0, part: int = 0) -> dict:
    part_key = jax.random.fold_in(jax.random.key(seed), part)
    key_grad, key_scale, key_mom, key_weight, key_rate = jax.random.split(part_key, 5)
    key_decay = jax.random.key(seed + 1)
    dev_scale = jax.random.uniform(key_scale, (DP_SIZE, 1, 1, 1), minval=0.5, maxval=2.0)
    grad_partial = jax.random.normal(key_grad, (DP_SIZE, MATS, ROWS, COLS)) * dev_scale * math.sqrt(DP_SIZE)
    momentum = jax.random.normal(key_mom, (MATS, ROWS, COLS))
    weight = 0.25 * jax.random.normal(key_weight, (MATS, ROWS, COLS))
    learn_rate = jax.random.uniform(key_rate, (MATS,), minval=0.1, maxval=1.0)
    decay_rate = jax.random.uniform(key_decay, (), minval=0.2, maxval=0.5)
    return {
        "grad_partial": grad_partial.astype(jnp.float32),
        "momentum": momentum.astype(jnp.float32),
        "weight": weight.astype(jnp.float32),
        "learn_rate": learn_rate.astype(jnp.float32),
        "decay_rate": decay_rate.astype(jnp.float32),
    }


def orthogonalize(update):
    upd_f32 = update.astype(jnp.float32)
    norm_val = jnp.sqrt(jnp.sum(upd_f32 * upd_f32))
    x_cur = (upd_f32 / (norm_val + NORM_EPS)).astype(jnp.bfloat16)
    if ROWS > COLS:
        x_cur = x_cur.T
    for step_idx in range(NS_STEPS):
        gram_mat = jnp.dot(x_cur, x_cur.T, preferred_element_type=jnp.float32).astype(jnp.bfloat16)
        gram_sq = jnp.dot(gram_mat, gram_mat, preferred_element_type=jnp.float32)
        poly_mat = (COEF_B * gram_mat.astype(jnp.float32) + COEF_C * gram_sq).astype(jnp.bfloat16)
        prod_mat = jnp.dot(poly_mat, x_cur, preferred_element_type=jnp.float32)
        x_cur = (COEF_A * x_cur.astype(jnp.float32) + prod_mat).astype(jnp.bfloat16)
    if ROWS > COLS:
        x_cur = x_cur.T
    return x_cur


def reference(grad_partial, momentum, weight, learn_rate, decay_rate):
    grad_mean = jnp.mean(grad_partial, axis=0)
    mom_new = MOMENTUM * momentum + grad_mean
    update = (grad_mean + MOMENTUM * mom_new).astype(jnp.bfloat16)
    ortho_mat = lax.map(orthogonalize, update)
    rate_col = learn_rate[:, None, None]
    weight_new = weight - rate_col * (OUT_SCALE * ortho_mat.astype(jnp.float32) + decay_rate * weight)
    return mom_new, weight_new, weight_new.astype(jnp.bfloat16)
```

```python
import math
import jax
import jax.numpy as jnp
from jax import lax
from jax.experimental import pallas as pl
from jax.experimental.pallas import tpu as pltpu
from jax.sharding import PartitionSpec as P

MOMENTUM = 0.95
NS_STEPS = 5
COEF_A = 3.4445
COEF_B = -4.7750
COEF_C = 2.0315
NORM_EPS = 1e-7
F32 = jnp.float32
BF16 = jnp.bfloat16

MATS, ROWS, COLS = 8, 1024, 2048
NC = 4
RC = 128 // NC
OUT_SCALE = 0.2 * math.sqrt(max(ROWS, COLS))


def dot_nt(lhs, rhs):
    return lax.dot_general(lhs, rhs, (((1,), (1,)), ((), ())), preferred_element_type=F32)


def dot_nn(lhs, rhs):
    return lax.dot_general(lhs, rhs, (((1,), (0,)), ((), ())), preferred_element_type=F32)


class Copies:
    def __init__(self, send_sems, recv_sems):
        self.send_sems, self.recv_sems = send_sems, recv_sems
        self.used = 0
        self.all = []

    def start(self, src, dst, **device):
        copy = pltpu.make_async_remote_copy(
            src_ref=src, dst_ref=dst, send_sem=self.send_sems.at[self.used], recv_sem=self.recv_sems.at[self.used],
            device_id=device, device_id_type=pl.DeviceIdType.MESH,
        )
        self.used += 1
        copy.start()
        self.all.append(copy)
        return copy


N_REMOTE = NC * (4 + 4 + 2 + 7 + 16) + 4 + 3 + 1 + 4 + 2 + 6
N_LOCAL = NC * 5 + 1 + 1 + 1 + 8 + 16


def muon_kernel(grad, mom, weight, rate, decay, mom_out, weight_out, full_out,
                own_g, sib_g, p2a, p1b, p1a, m2b, m1a, m1b, mom_v, upd, gath, sq_acc, x_cur, gram, poly,
                w_full, x_full, w_new, w_low, send_sems, recv_sems, local_sems):
    me = lax.axis_index("dp")
    tp = lax.axis_index("tp")
    x, core = lax.div(me, 2), lax.rem(me, 2)
    z, y = lax.div(tp, 4), lax.rem(tp, 4)
    xp, xm, x2 = lax.rem(x + 1, 4), lax.rem(x + 3, 4), lax.rem(x + 2, 4)
    yp, ym = lax.rem(y + 1, 4), lax.rem(y + 3, 4)
    zp, zm = lax.rem(z + 1, 4), lax.rem(z + 3, 4)
    sib = x * 2 + 1 - core
    dp_xp, dp_xm, dp_x2 = xp * 2 + core, xm * 2 + core, x2 * 2 + core
    tp_yp, tp_ym, tp_zp, tp_zm = z * 4 + yp, z * 4 + ym, zp * 4 + y, zm * 4 + y
    slots = (x2, xp, xm, x)

    rem = Copies(send_sems, recv_sems)
    n_local = [0]
    open_local = []

    def local(src, dst):
        copy = pltpu.make_async_copy(src, dst, local_sems.at[n_local[0]])
        n_local[0] += 1
        copy.start()
        return copy

    own_loads = {}
    for r in range(NC):
        for s in range(4):
            row = pl.multiple_of((slots[s] * 2 + core) * 128 + r * RC, RC)
            own_loads[r, s] = local(grad.at[0, :, pl.ds(row, RC), :], own_g.at[s, r])
    mom_load = local(mom, mom_v)

    barrier = pltpu.get_barrier_semaphore()
    for i in range(1, 8):
        pl.semaphore_signal(barrier, inc=1, device_id={"dp": lax.rem(me + i, 8)}, device_id_type=pl.DeviceIdType.MESH)
    for t in (tp_yp, tp_ym, tp_zp, tp_zm):
        pl.semaphore_signal(barrier, inc=1, device_id={"tp": t}, device_id_type=pl.DeviceIdType.MESH)
    pl.semaphore_wait(barrier, 11)

    d2d = {}
    for r in range(NC):
        for s in range(4):
            row = pl.multiple_of((slots[s] * 2 + 1 - core) * 128 + r * RC, RC)
            d2d[r, s] = rem.start(grad.at[0, :, pl.ds(row, RC), :], sib_g.at[s, r], dp=sib)

    st = {}

    def rs_raw(r):
        for s in (0, 1, 2):
            own_loads[r, s].wait()
            d2d[r, s].wait_recv()
            own_g[s, r] = own_g[s, r] + sib_g[s, r]
            if s == 0:
                st["p2a", r] = rem.start(own_g.at[0, r, pl.ds(0, 4)], p2a.at[r], dp=dp_xp)
                st["m2b", r] = rem.start(own_g.at[0, r, pl.ds(4, 4)], m2b.at[r], dp=dp_xm)
            if s == 1:
                st["p1b", r] = rem.start(own_g.at[1, r, pl.ds(4, 4)], p1b.at[r], dp=dp_xp)
            if s == 2:
                st["m1a", r] = rem.start(own_g.at[2, r, pl.ds(0, 4)], m1a.at[r], dp=dp_xm)

    def rs_sum(r):
        st["p2a", r].wait_recv()
        own_g[1, r, pl.ds(0, 4)] = own_g[1, r, pl.ds(0, 4)] + p2a[r]
        st["p1a", r] = rem.start(own_g.at[1, r, pl.ds(0, 4)], p1a.at[r], dp=dp_xp)
        st["m2b", r].wait_recv()
        own_g[2, r, pl.ds(4, 4)] = own_g[2, r, pl.ds(4, 4)] + m2b[r]
        st["m1b", r] = rem.start(own_g.at[2, r, pl.ds(4, 4)], m1b.at[r], dp=dp_xm)

    def update(r):
        own_loads[r, 3].wait()
        d2d[r, 3].wait_recv()
        if r == 0:
            mom_load.wait()
        for name in ("p1b", "m1a", "p1a", "m1b"):
            st[name, r].wait_recv()
        for half, (near, far) in enumerate(((m1a, p1a), (p1b, m1b))):
            js = pl.ds(half * 4, 4)
            total = (own_g[3, r, js] + sib_g[3, r, js]) + (near[r] + far[r])
            mean = total * (1.0 / 8.0)
            mom_new = MOMENTUM * mom_v[js, pl.ds(r * RC, RC)] + mean
            mom_v[js, pl.ds(r * RC, RC)] = mom_new
            upd[r, js] = (mean + MOMENTUM * mom_new).astype(BF16)
        st["own", r] = local(upd.at[r, me], gath.at[z, y, r, me])
        st["a2a", r] = [rem.start(upd.at[r, lax.rem(me + i, 8)], gath.at[z, y, r, me], dp=lax.rem(me + i, 8))
                        for i in range(1, 8)]

    lo, hi = pl.ds(0, 4), pl.ds(4, 4)

    def both(name, r, block, **axes):
        for key, device in axes.items():
            axis = "tp"
            st[name + key, r] = rem.start(block, block, **{axis: device})

    def gather1(r):
        st["own", r].wait()
        for copy in st["a2a", r]:
            copy.wait_recv()
        both("g1z", r, gath.at[z, y, r, lo], p=tp_zp, m=tp_zm)
        both("g1y", r, gath.at[z, y, r, hi], p=tp_yp, m=tp_ym)

    def forward1(r):
        st["g1zp", r].wait_recv()
        both("f1z", r, gath.at[zm, y, r, pl.ds(0, 2)], p=tp_zp)
        st["g1yp", r].wait_recv()
        both("f1y", r, gath.at[z, ym, r, pl.ds(4, 2)], p=tp_yp)
        st["g1zm", r].wait_recv()
        both("f1z", r, gath.at[zp, y, r, pl.ds(2, 2)], m=tp_zm)
        st["g1ym", r].wait_recv()
        both("f1y", r, gath.at[z, yp, r, pl.ds(6, 2)], m=tp_ym)

    def gather2(r):
        st["f1zp", r].wait_recv()
        st["f1zm", r].wait_recv()
        both("g2y", r, gath.at[:, y, r, lo], p=tp_yp, m=tp_ym)
        st["f1yp", r].wait_recv()
        st["f1ym", r].wait_recv()
        both("g2z", r, gath.at[z, :, r, hi], p=tp_zp, m=tp_zm)

    def forward2(r):
        st["g2yp", r].wait_recv()
        both("f2y", r, gath.at[:, ym, r, pl.ds(0, 2)], p=tp_yp)
        st["g2ym", r].wait_recv()
        both("f2y", r, gath.at[:, yp, r, pl.ds(2, 2)], m=tp_ym)
        st["g2zp", r].wait_recv()
        both("f2z", r, gath.at[zm, :, r, pl.ds(4, 2)], p=tp_zp)
        st["g2zm", r].wait_recv()
        both("f2z", r, gath.at[zp, :, r, pl.ds(6, 2)], m=tp_zm)

    def squares(r):
        for name in ("f2yp", "f2ym", "f2zp", "f2zm"):
            st[name, r].wait_recv()
        if r == 0:
            sq_acc[...] = jnp.zeros_like(sq_acc)

        @pl.loop(0, 4)
        def _(i):
            for j in range(4):
                block = gath[i, j, r].astype(F32)
                sq_acc[...] += jnp.sum((block * block).reshape(RC, 8, 128), axis=0)

    stages = (rs_raw, rs_sum, update, gather1, forward1, gather2, forward2, squares)
    for slot in range(NC + len(stages) - 1):
        for s, stage in enumerate(stages):
            if 0 <= slot - s < NC:
                stage(slot - s)

    mom_store = local(mom_v, mom_out)
    w_own = local(weight, w_full.at[:, me])
    w_send = [rem.start(weight, w_full.at[:, me], dp=d) for d in (dp_xp, dp_xm, dp_x2, sib)]
    base = rem.used
    w_fwd = []

    norm = jnp.sqrt(jnp.sum(sq_acc[...], keepdims=True))
    inv = 1.0 / (norm + NORM_EPS)

    @pl.loop(0, 4)
    def _(i):
        for j in range(4):
            cols = pl.ds(pl.multiple_of(i * 512 + j * 128, 128), 128)
            for r in range(NC):
                for d in range(8):
                    block = gath[i, j, r, d].astype(F32) * inv
                    x_cur[pl.ds(d * 128 + r * RC, RC), cols] = block.astype(BF16)

    def mirror_store(dst, block, first):
        dst[pl.ds(first, ROWS - first), pl.ds(first, 256)] = block
        if first + 256 < ROWS:
            dst[pl.ds(first, 256), pl.ds(first + 256, ROWS - first - 256)] = block[256:, :].T

    def polynomial():
        for first in range(0, ROWS, 256):
            below = pl.ds(first, ROWS - first)
            mirror_store(gram, dot_nt(x_cur[below, :], x_cur[pl.ds(first, 256), :]).astype(BF16), first)
        for first in range(0, ROWS, 256):
            below, cols = pl.ds(first, ROWS - first), pl.ds(first, 256)
            square = dot_nn(gram[below, :], gram[:, cols])
            mirror_store(poly, (COEF_B * gram[below, cols].astype(F32) + COEF_C * square).astype(BF16), first)

    @pl.loop(0, NS_STEPS - 1)
    def _(step):
        polynomial()
        for first in range(0, COLS, 256):
            cols = pl.ds(first, 256)
            block = x_cur[:, cols]
            prod = dot_nn(poly[...], block)
            x_cur[:, cols] = (COEF_A * block.astype(F32) + prod).astype(BF16)

    for i, d in enumerate((dp_xm, dp_xp, dp_x2)):
        w_send[i].wait_recv()
        w_fwd.append(rem.start(w_full.at[:, d], w_full.at[:, d], dp=sib))

    polynomial()
    own_cols = pl.ds(pl.multiple_of(tp * 128, 128), 128)
    block = x_cur[:, own_cols]
    x_full[me] = (COEF_A * block.astype(F32) + dot_nn(poly[...], block)).astype(BF16)

    top, bot = pl.ds(0, 512), pl.ds(512, 512)
    f_pt = rem.start(x_full.at[me, top], x_full.at[me, top], dp=dp_xp)
    f_mb = rem.start(x_full.at[me, bot], x_full.at[me, bot], dp=dp_xm)
    f_pb = rem.start(x_full.at[me, bot], x_full.at[me, bot], dp=dp_xp)
    f_mt = rem.start(x_full.at[me, top], x_full.at[me, top], dp=dp_xm)
    f_s = rem.start(x_full.at[me], x_full.at[me], dp=sib)

    w_own.wait()
    w_send[3].wait_recv()
    for copy in w_fwd:
        copy.wait_recv()
    stores = []

    def finish(mat):
        lr = rate[mat]
        dec = decay[0]
        wf = w_full[mat].reshape(ROWS, 128)
        new = wf - lr * (OUT_SCALE * x_full[mat].astype(F32) + dec * wf)
        w_low[mat] = new.astype(BF16)
        stores.append(local(w_low.at[mat], full_out.at[mat]))
        wo = w_full[mat, me]
        rows = pl.ds(pl.multiple_of(me * 128, 128), 128)
        w_new[mat] = wo - lr * (OUT_SCALE * x_full[mat, rows].astype(F32) + dec * wo)

    finish(me)
    f_pt.wait_recv()
    q_p = rem.start(x_full.at[dp_xm, top], x_full.at[dp_xm, top], dp=dp_xp)
    f_mb.wait_recv()
    q_m = rem.start(x_full.at[dp_xp, bot], x_full.at[dp_xp, bot], dp=dp_xm)
    f_s.wait_recv()
    finish(sib)
    f_pb.wait_recv()
    s_m = rem.start(x_full.at[dp_xm], x_full.at[dp_xm], dp=sib)
    f_mt.wait_recv()
    s_p = rem.start(x_full.at[dp_xp], x_full.at[dp_xp], dp=sib)
    finish(dp_xm)
    finish(dp_xp)
    s_m.wait_recv()
    finish(xm * 2 + 1 - core)
    s_p.wait_recv()
    finish(xp * 2 + 1 - core)
    q_p.wait_recv()
    s_t = rem.start(x_full.at[dp_x2, top], x_full.at[dp_x2, top], dp=sib)
    q_m.wait_recv()
    s_b = rem.start(x_full.at[dp_x2, bot], x_full.at[dp_x2, bot], dp=sib)
    finish(dp_x2)
    s_t.wait_recv()
    s_b.wait_recv()
    finish(x2 * 2 + 1 - core)
    stores.append(local(w_new, weight_out))
    for copy in rem.all:
        copy.wait_send()
    mom_store.wait()
    for copy in stores:
        copy.wait()


def solution(mesh):
    def local_step(grad_local, mom_local, weight_local, learn_rate, decay_rate):
        hbm = pl.BlockSpec(memory_space=pl.ANY)
        smem = pl.BlockSpec(memory_space=pltpu.SMEM)
        V = pltpu.VMEM
        return pl.pallas_call(
            muon_kernel,
            out_shape=(
                jax.ShapeDtypeStruct((8, 128, 128), F32),
                jax.ShapeDtypeStruct((8, 128, 128), F32),
                jax.ShapeDtypeStruct((8, 1024, 128), BF16),
            ),
            in_specs=[hbm, hbm, hbm, smem, smem],
            out_specs=(hbm, hbm, hbm),
            scratch_shapes=[
                V((4, NC, 8, RC, 128), F32), V((4, NC, 8, RC, 128), F32),
                V((NC, 4, RC, 128), F32), V((NC, 4, RC, 128), F32), V((NC, 4, RC, 128), F32),
                V((NC, 4, RC, 128), F32), V((NC, 4, RC, 128), F32), V((NC, 4, RC, 128), F32),
                V((8, 128, 128), F32), V((NC, 8, RC, 128), BF16),
                V((4, 4, NC, 8, RC, 128), BF16), V((8, 128), F32),
                V((ROWS, COLS), BF16), V((ROWS, ROWS), BF16), V((ROWS, ROWS), BF16),
                V((8, 8, 128, 128), F32), V((8, ROWS, 128), BF16), V((8, 128, 128), F32), V((8, ROWS, 128), BF16),
                pltpu.SemaphoreType.DMA((N_REMOTE,)), pltpu.SemaphoreType.DMA((N_REMOTE,)),
                pltpu.SemaphoreType.DMA((N_LOCAL,)),
            ],
            compiler_params=pltpu.CompilerParams(
                collective_id=0, has_side_effects=True, vmem_limit_bytes=58 * 2**20),
            name="muon_step",
        )(grad_local, mom_local, weight_local, learn_rate, decay_rate.reshape(1))

    return jax.shard_map(
        local_step,
        mesh=mesh,
        in_specs=(P(("rep", "dp"), None, None, "tp"), P("rep", "dp", "tp"), P("rep", "dp", "tp"), P("rep"), P()),
        out_specs=(P("rep", "dp", "tp"), P("rep", "dp", "tp"), P("rep", None, "tp")),
        check_vma=False,
    )
```

```python
import math
import jax
import jax.numpy as jnp
from jax import lax
from jax.experimental import pallas as pl
from jax.experimental.pallas import tpu as pltpu
from jax.sharding import PartitionSpec as P

MOMENTUM = 0.95
NS_STEPS = 5
COEF_A = 3.4445
COEF_B = -4.7750
COEF_C = 2.0315
NORM_EPS = 1e-7
F32 = jnp.float32
BF16 = jnp.bfloat16

MATS, ROWS, COLS = 8, 1024, 2048
NC = 8
RC = 128 // NC
OUT_SCALE = 0.2 * math.sqrt(max(ROWS, COLS))


def dot_nt(lhs, rhs):
    return lax.dot_general(lhs, rhs, (((1,), (1,)), ((), ())), preferred_element_type=F32)


def dot_nn(lhs, rhs):
    return lax.dot_general(lhs, rhs, (((1,), (0,)), ((), ())), preferred_element_type=F32)


ORDER = (
    ("dd", 0), ("dd", 1), ("dd", 2), ("dd", 3), ("far", 0), ("far", 1), ("near", 1), ("near", 0), ("dd", 4),
    ("far", 2), ("sum", 0), ("far", 3), ("sum", 1), ("near", 2), ("dd", 6), ("sum", 2), ("update", 0), ("far", 4),
    ("near", 3), ("sum", 3), ("update", 1), ("update", 2), ("dd", 5), ("near", 4), ("dd", 7), ("sum", 4), ("far", 5),
    ("gather1", 0), ("update", 3), ("near", 5), ("far", 6), ("gather1", 1), ("gather1", 2), ("near", 6), ("far", 7),
    ("sum", 5), ("gather2", 0), ("gather1", 3), ("update", 4), ("sum", 6), ("gather2", 1), ("near", 7), ("sum", 7),
    ("update", 5), ("gather2", 2), ("gather1", 4), ("forward2", 0), ("update", 6), ("gather2", 3), ("update", 7),
    ("gather1", 5), ("forward2", 2), ("gather1", 6), ("forward2", 1), ("gather1", 7), ("gather2", 4), ("gather2", 5),
    ("gather2", 6), ("gather2", 7), ("squares", 0), ("forward2", 5), ("forward2", 3), ("forward2", 4),
    ("forward2", 6), ("forward2", 7), ("squares", 1), ("squares", 5), ("squares", 4), ("squares", 2), ("squares", 6),
    ("squares", 3), ("squares", 7),
)

CHUNK_GROUPS = ("dd0", "dd1", "p2", "p1", "a2a", "g1", "g2", "f2")
LATE_GROUPS = ("w3", "w4", "fa", "fb", "fs", "s1", "q", "s2")
SEND_GROUPS = ("dd", "rs", "a2a", "g1", "g2", "f2", "w3", "w4", "last")
N_RECV = NC * len(CHUNK_GROUPS) + len(LATE_GROUPS)
N_LOCAL = NC + 2


def muon_kernel(grad, mom, weight, rate, decay, mom_out, weight_out, full_out,
                own_g, sib_g, p2a, p1b, p1a, m2b, m1a, m1b, upd, gath, sq_acc, x_cur, gram, poly,
                w_full, x_full, send_sems, recv_sems, local_sems):
    me = lax.axis_index("dp")
    tp = lax.axis_index("tp")
    x, core = lax.div(me, 2), lax.rem(me, 2)
    z, y = lax.div(tp, 4), lax.rem(tp, 4)
    xp, xm, x2 = lax.rem(x + 1, 4), lax.rem(x + 3, 4), lax.rem(x + 2, 4)
    yp, ym, y2 = lax.rem(y + 1, 4), lax.rem(y + 3, 4), lax.rem(y + 2, 4)
    zp, zm, z2 = lax.rem(z + 1, 4), lax.rem(z + 3, 4), lax.rem(z + 2, 4)
    sib = x * 2 + 1 - core
    dp_xp, dp_xm, dp_x2 = xp * 2 + core, xm * 2 + core, x2 * 2 + core
    tp_yp, tp_ym, tp_y2 = z * 4 + yp, z * 4 + ym, z * 4 + y2
    tp_zp, tp_zm, tp_z2 = zp * 4 + y, zm * 4 + y, z2 * 4 + y
    slots = (x2, xp, xm, x)

    def recv_sem(group, r=None):
        if r is None:
            return recv_sems.at[NC * len(CHUNK_GROUPS) + LATE_GROUPS.index(group)]
        return recv_sems.at[r * len(CHUNK_GROUPS) + CHUNK_GROUPS.index(group)]

    def send(src, dst, sent, group, r=None, **device):
        pltpu.make_async_remote_copy(
            src_ref=src, dst_ref=dst, send_sem=send_sems.at[SEND_GROUPS.index(sent)], recv_sem=recv_sem(group, r),
            device_id=device, device_id_type=pl.DeviceIdType.MESH,
        ).start()

    def drain(sem, like):
        pltpu.make_async_copy(like, like, sem).wait()

    def arrived(like, group, r=None):
        drain(recv_sem(group, r), like)

    for r in range(NC):
        for s in range(4):
            row = pl.multiple_of((slots[s] * 2 + core) * 128 + r * RC, RC)
            pltpu.make_async_copy(grad.at[0, :, pl.ds(row, RC), :], own_g.at[s, r], local_sems.at[r]).start()
    mom_load = pltpu.make_async_copy(mom, mom_out, local_sems.at[NC])
    mom_load.start()

    barrier = pltpu.get_barrier_semaphore()
    for i in range(1, 8):
        pl.semaphore_signal(barrier, inc=1, device_id={"dp": lax.rem(me + i, 8)}, device_id_type=pl.DeviceIdType.MESH)
    for t in (tp_yp, tp_ym, tp_y2, tp_zp, tp_zm, tp_z2):
        pl.semaphore_signal(barrier, inc=1, device_id={"tp": t}, device_id_type=pl.DeviceIdType.MESH)
    with jax.named_scope("entry"):
        pl.semaphore_wait(barrier, 13)

    def dd(r):
        for s in range(4):
            row = pl.multiple_of((slots[s] * 2 + 1 - core) * 128 + r * RC, RC)
            send(grad.at[0, :, pl.ds(row, RC), :], sib_g.at[s, r], "dd", "dd1" if s else "dd0", r, dp=sib)

    lo, hi = pl.ds(0, 4), pl.ds(4, 4)

    def far(r):
        drain(local_sems.at[r], own_g.at[:, r])
        arrived(sib_g.at[0, r], "dd0", r)
        own_g[0, r] = own_g[0, r] + sib_g[0, r]
        send(own_g.at[0, r, lo], p2a.at[r], "rs", "p2", r, dp=dp_xp)
        send(own_g.at[0, r, hi], m2b.at[r], "rs", "p2", r, dp=dp_xm)

    def near(r):
        arrived(sib_g.at[pl.ds(1, 3), r], "dd1", r)
        own_g[1, r] = own_g[1, r] + sib_g[1, r]
        send(own_g.at[1, r, hi], p1b.at[r], "rs", "p1", r, dp=dp_xp)
        own_g[2, r] = own_g[2, r] + sib_g[2, r]
        send(own_g.at[2, r, lo], m1a.at[r], "rs", "p1", r, dp=dp_xm)

    def sum_(r):
        arrived(own_g.at[0, r], "p2", r)
        own_g[1, r, lo] = own_g[1, r, lo] + p2a[r]
        send(own_g.at[1, r, lo], p1a.at[r], "rs", "p1", r, dp=dp_xp)
        own_g[2, r, hi] = own_g[2, r, hi] + m2b[r]
        send(own_g.at[2, r, hi], m1b.at[r], "rs", "p1", r, dp=dp_xm)

    waited = []

    def update(r):
        if not waited:
            mom_load.wait()
            waited.append(r)
        arrived(own_g.at[pl.ds(0, 2), r], "p1", r)
        for half, (near_ref, far_ref) in enumerate(((m1a, p1a), (p1b, m1b))):
            js = pl.ds(half * 4, 4)
            total = (own_g[3, r, js] + sib_g[3, r, js]) + (near_ref[r] + far_ref[r])
            mean = total * (1.0 / 8.0)
            mom_new = MOMENTUM * mom_out[js, pl.ds(r * RC, RC)] + mean
            mom_out[js, pl.ds(r * RC, RC)] = mom_new
            upd[r, js] = (mean + MOMENTUM * mom_new).astype(BF16)
        for i in range(1, 8):
            to = lax.rem(me + i, 8)
            send(upd.at[r, to], gath.at[z, y, r, me], "a2a", "a2a", r, dp=to)
        gath[z, y, r, me] = upd[r, me]

    def gather1(r):
        arrived(upd.at[r, pl.ds(0, 7)], "a2a", r)
        for near_first in ((tp_zp, tp_yp), (tp_zm, tp_ym), (tp_z2, tp_y2)):
            send(gath.at[z, y, r, lo], gath.at[z, y, r, lo], "g1", "g1", r, tp=near_first[0])
            send(gath.at[z, y, r, hi], gath.at[z, y, r, hi], "g1", "g1", r, tp=near_first[1])

    def gather2(r):
        arrived(gath.at[0, pl.ds(0, 3), r], "g1", r)
        for t in (tp_yp, tp_ym):
            send(gath.at[:, y, r, lo], gath.at[:, y, r, lo], "g2", "g2", r, tp=t)
        for t in (tp_zp, tp_zm):
            send(gath.at[z, :, r, hi], gath.at[z, :, r, hi], "g2", "g2", r, tp=t)

    def forward2(r):
        arrived(gath.at[pl.ds(0, 2), :, r], "g2", r)
        for block, t in ((gath.at[:, ym, r, pl.ds(0, 2)], tp_yp), (gath.at[:, yp, r, pl.ds(2, 2)], tp_ym),
                         (gath.at[zm, :, r, pl.ds(4, 2)], tp_zp), (gath.at[zp, :, r, pl.ds(6, 2)], tp_zm)):
            send(block, block, "f2", "f2", r, tp=t)

    def squares(r):
        arrived(gath.at[0, :, r], "f2", r)

        @pl.loop(0, 4)
        def _(i):
            for j in range(4):
                block = gath[i, j, r].astype(F32)
                sq_acc[...] += jnp.sum((block * block).reshape(RC, 8, 128), axis=0)

    sq_acc[...] = jnp.zeros_like(sq_acc)
    stages = {"dd": dd, "far": far, "near": near, "sum": sum_, "update": update, "gather1": gather1,
              "gather2": gather2, "forward2": forward2, "squares": squares}
    for name, r in ORDER:
        with jax.named_scope(f"{name}_{r}"):
            stages[name](r)

    w_own = pltpu.make_async_copy(weight, w_full.at[:, me], local_sems.at[NC + 1])
    w_own.start()
    for d in (dp_xp, dp_xm, dp_x2):
        send(weight, w_full.at[:, me], "w3", "w3", dp=d)
    send(weight, w_full.at[:, me], "w4", "w4", dp=sib)

    norm = jnp.sqrt(jnp.sum(sq_acc[...], keepdims=True))
    inv = 1.0 / (norm + NORM_EPS)

    @pl.loop(0, 4)
    def _(i):
        for j in range(4):
            cols = pl.ds(pl.multiple_of(i * 512 + j * 128, 128), 128)
            for r in range(NC):
                for d in range(8):
                    block = gath[i, j, r, d].astype(F32) * inv
                    x_cur[pl.ds(d * 128 + r * RC, RC), cols] = block.astype(BF16)

    def mirror_store(dst, block, first):
        dst[pl.ds(first, ROWS - first), pl.ds(first, 256)] = block
        if first + 256 < ROWS:
            dst[pl.ds(first, 256), pl.ds(first + 256, ROWS - first - 256)] = block[256:, :].T

    def polynomial():
        for first in range(0, ROWS, 256):
            below = pl.ds(first, ROWS - first)
            mirror_store(gram, dot_nt(x_cur[below, :], x_cur[pl.ds(first, 256), :]).astype(BF16), first)
        for first in range(0, ROWS, 256):
            below, cols = pl.ds(first, ROWS - first), pl.ds(first, 256)
            square = dot_nn(gram[below, :], gram[:, cols])
            mirror_store(poly, (COEF_B * gram[below, cols].astype(F32) + COEF_C * square).astype(BF16), first)

    @pl.loop(0, NS_STEPS - 1)
    def _(step):
        polynomial()
        for first in range(0, COLS, 256):
            cols = pl.ds(first, 256)
            block = x_cur[:, cols]
            prod = dot_nn(poly[...], block)
            x_cur[:, cols] = (COEF_A * block.astype(F32) + prod).astype(BF16)

    arrived(w_full.at[:, pl.ds(0, 3)], "w3")
    for d in (dp_xm, dp_xp, dp_x2):
        send(w_full.at[:, d], w_full.at[:, d], "w4", "w4", dp=sib)

    polynomial()
    own_cols = pl.ds(pl.multiple_of(tp * 128, 128), 128)
    top, bot = pl.ds(0, 512), pl.ds(512, 512)
    block = x_cur[:, own_cols]

    def last(group, src, **device):
        send(src, src, "last", group, **device)

    for rows, first, second in ((top, dp_xp, "fa"), (bot, dp_xm, "fa")):
        x_full[me, rows] = (COEF_A * x_cur[rows, own_cols].astype(F32) + dot_nn(poly[rows, :], block)).astype(BF16)
        last(second, x_full.at[me, rows], dp=first)
    last("fb", x_full.at[me, bot], dp=dp_xp)
    last("fb", x_full.at[me, top], dp=dp_xm)
    last("fs", x_full.at[me], dp=sib)

    w_own.wait()
    arrived(w_full.at[:, pl.ds(0, 4)], "w4")

    def finish(mat):
        lr = rate[mat]
        dec = decay[0]
        wf = w_full[mat].reshape(ROWS, 128)
        new = wf - lr * (OUT_SCALE * x_full[mat].astype(F32) + dec * wf)
        full_out[mat] = new.astype(BF16)
        wo = w_full[mat, me]
        rows = pl.ds(pl.multiple_of(me * 128, 128), 128)
        weight_out[mat] = wo - lr * (OUT_SCALE * x_full[mat, rows].astype(F32) + dec * wo)

    pair = x_full.at[0]
    finish(me)
    arrived(pair, "fa")
    last("q", x_full.at[dp_xm, top], dp=dp_xp)
    last("q", x_full.at[dp_xp, bot], dp=dp_xm)
    arrived(pair, "fs")
    finish(sib)
    arrived(pair, "fb")
    last("s1", x_full.at[dp_xm], dp=sib)
    last("s1", x_full.at[dp_xp], dp=sib)
    finish(dp_xm)
    finish(dp_xp)
    arrived(x_full.at[pl.ds(0, 2)], "s1")
    finish(xm * 2 + 1 - core)
    finish(xp * 2 + 1 - core)
    arrived(pair, "q")
    last("s2", x_full.at[dp_x2, top], dp=sib)
    last("s2", x_full.at[dp_x2, bot], dp=sib)
    finish(dp_x2)
    arrived(pair, "s2")
    finish(x2 * 2 + 1 - core)

    with jax.named_scope("sends"):
        for group, like in (("dd", own_g), ("rs", own_g.at[pl.ds(0, 3)]), ("a2a", upd.at[:, pl.ds(0, 7)]),
                            ("g1", gath.at[0, pl.ds(0, 3)]), ("g2", gath.at[pl.ds(0, 2)]), ("f2", gath.at[0]),
                            ("w3", w_full.at[:, pl.ds(0, 3)]), ("w4", w_full.at[:, pl.ds(0, 4)]),
                            ("last", x_full.at[pl.ds(0, 7)])):
            drain(send_sems.at[SEND_GROUPS.index(group)], like)


def solution(mesh):
    def local_step(grad_local, mom_local, weight_local, learn_rate, decay_rate):
        hbm = pl.BlockSpec(memory_space=pltpu.HBM)
        vmem = pl.BlockSpec(memory_space=pltpu.VMEM)
        smem = pl.BlockSpec(memory_space=pltpu.SMEM)
        V = pltpu.VMEM
        return pl.pallas_call(
            muon_kernel,
            out_shape=(
                V((8, 128, 128), F32),
                V((8, 128, 128), F32),
                V((8, 1024, 128), BF16),
            ),
            in_specs=[hbm, hbm, hbm, smem, smem],
            out_specs=(vmem, vmem, vmem),
            scratch_shapes=[
                V((4, NC, 8, RC, 128), F32), V((4, NC, 8, RC, 128), F32),
                V((NC, 4, RC, 128), F32), V((NC, 4, RC, 128), F32), V((NC, 4, RC, 128), F32),
                V((NC, 4, RC, 128), F32), V((NC, 4, RC, 128), F32), V((NC, 4, RC, 128), F32),
                V((NC, 8, RC, 128), BF16),
                V((4, 4, NC, 8, RC, 128), BF16), V((8, 128), F32),
                V((ROWS, COLS), BF16), V((ROWS, ROWS), BF16), V((ROWS, ROWS), BF16),
                V((8, 8, 128, 128), F32), V((8, ROWS, 128), BF16),
                pltpu.SemaphoreType.DMA((len(SEND_GROUPS),)), pltpu.SemaphoreType.DMA((N_RECV,)),
                pltpu.SemaphoreType.DMA((N_LOCAL,)),
            ],
            compiler_params=pltpu.CompilerParams(
                collective_id=0, has_side_effects=True, vmem_limit_bytes=63_400_000),
            name="muon_step",
        )(grad_local, mom_local, weight_local, learn_rate, decay_rate.reshape(1))

    return jax.shard_map(
        local_step,
        mesh=mesh,
        in_specs=(P(("rep", "dp"), None, None, "tp"), P("rep", "dp", "tp"), P("rep", "dp", "tp"), P("rep"), P()),
        out_specs=(P("rep", "dp", "tp"), P("rep", "dp", "tp"), P("rep", None, "tp")),
        check_vma=False,
    )
```

```python
import math
import jax
import jax.numpy as jnp
from jax import lax
from jax.experimental import pallas as pl
from jax.experimental.pallas import tpu as pltpu
from jax.sharding import PartitionSpec as P

MOMENTUM = 0.95
NS_STEPS = 5
COEF_A = 3.4445
COEF_B = -4.7750
COEF_C = 2.0315
NORM_EPS = 1e-7
F32 = jnp.float32
BF16 = jnp.bfloat16

MATS, ROWS, COLS = 8, 1024, 2048
NC = 8
RC = 128 // NC
CR = 8 * RC
OUT_SCALE = 0.2 * math.sqrt(max(ROWS, COLS))


def dot_nt(lhs, rhs):
    return lax.dot_general(lhs, rhs, (((1,), (1,)), ((), ())), preferred_element_type=F32)


def dot_nn(lhs, rhs):
    return lax.dot_general(lhs, rhs, (((1,), (0,)), ((), ())), preferred_element_type=F32)


ORDER = (
    ("mom", 0), ("dd", 4), ("mom", 1), ("dd", 0), ("dd", 2), ("mom", 2), ("dd", 1), ("far", 0), ("dd", 5),
    ("near", 0), ("far", 2), ("far", 1), ("dd", 7), ("near", 2), ("near", 1), ("sum", 0), ("dd", 3), ("far", 4),
    ("sum", 2), ("sum", 1), ("far", 5), ("near", 5), ("far", 3), ("far", 7), ("gather1", 0), ("near", 3),
    ("gather1", 2), ("mom", 3), ("dd", 6), ("far", 6), ("mom", 4), ("gather1", 1), ("sum", 3), ("gather2", 0),
    ("near", 4), ("mom", 5), ("sum", 4), ("sum", 5), ("gather2", 2), ("near", 6), ("gather2", 1), ("gather1", 3),
    ("mom", 6), ("forward2", 0), ("mom", 7), ("sum", 6), ("near", 7), ("forward2", 2), ("sum", 7), ("gather1", 4),
    ("gather1", 5), ("forward2", 1), ("gather2", 3), ("gather1", 6), ("gather1", 7), ("gather2", 4), ("gather2", 5),
    ("gather2", 6), ("gather2", 7), ("forward2", 3), ("norm", 0), ("forward2", 5), ("scale", 2), ("scale", 1),
    ("forward2", 4), ("forward2", 6), ("scale", 0), ("gram", 0), ("forward2", 7), ("scale", 3), ("gram", 1),
    ("scale", 5), ("scale", 4), ("gram", 2), ("scale", 6), ("scale", 7), ("gram", 3),
)

CHUNK_GROUPS = ("dd0", "dd1", "p2", "p1", "mom", "g1", "g2", "f2")
LATE_GROUPS = ("sq", "back", "w3", "w4", "fa", "fb", "fs", "s1", "q", "s2")
SEND_GROUPS = ("dd", "rs", "mom", "back", "sq", "g1", "g2", "f2", "w3", "w4", "last")
N_RECV = NC * len(CHUNK_GROUPS) + len(LATE_GROUPS)
N_LOCAL = NC + 2


def muon_kernel(grad, mom, weight, rate, decay, mom_out, weight_out, full_out,
                own_g, sib_g, p2a, p1b, p1a, m2b, m1a, m1b, mom_x, mom_y, mom_r, gath, sq_own, sq_all,
                x_cur, gram, poly, w_full, x_full, send_sems, recv_sems, local_sems):
    me = lax.axis_index("dp")
    tp = lax.axis_index("tp")
    x, core = lax.div(me, 2), lax.rem(me, 2)
    z, y = lax.div(tp, 4), lax.rem(tp, 4)
    xp, xm, x2 = lax.rem(x + 1, 4), lax.rem(x + 3, 4), lax.rem(x + 2, 4)
    yp, ym, y2 = lax.rem(y + 1, 4), lax.rem(y + 3, 4), lax.rem(y + 2, 4)
    zp, zm, z2 = lax.rem(z + 1, 4), lax.rem(z + 3, 4), lax.rem(z + 2, 4)
    sib = x * 2 + 1 - core
    dp_xp, dp_xm, dp_x2 = xp * 2 + core, xm * 2 + core, x2 * 2 + core
    tp_yp, tp_ym, tp_y2 = z * 4 + yp, z * 4 + ym, z * 4 + y2
    tp_zp, tp_zm, tp_z2 = zp * 4 + y, zm * 4 + y, z2 * 4 + y
    slots = (x2, xp, xm, x)

    def recv_sem(group, r=None):
        if r is None:
            return recv_sems.at[NC * len(CHUNK_GROUPS) + LATE_GROUPS.index(group)]
        return recv_sems.at[r * len(CHUNK_GROUPS) + CHUNK_GROUPS.index(group)]

    def send(src, dst, sent, group, r=None, **device):
        pltpu.make_async_remote_copy(
            src_ref=src, dst_ref=dst, send_sem=send_sems.at[SEND_GROUPS.index(sent)], recv_sem=recv_sem(group, r),
            device_id=device, device_id_type=pl.DeviceIdType.MESH,
        ).start()

    def drain(sem, like):
        pltpu.make_async_copy(like, like, sem).wait()

    def arrived(like, group, r=None):
        drain(recv_sem(group, r), like)

    def peers(rest=7):
        return [lax.rem(me + i, 8) for i in range(1, rest + 1)]

    tp_peers = [lax.rem(tp + i, 16) for i in range(1, 16)]

    for r in range(NC):
        for s in range(4):
            pltpu.make_async_copy(grad.at[slots[s] * 2 + core, :, pl.ds(r * RC, RC), :], own_g.at[s, r],
                                  local_sems.at[r]).start()
        pltpu.make_async_copy(mom.at[me, pl.ds(r * RC, RC), :], mom_x.at[r, me], local_sems.at[NC]).start()

    barrier = pltpu.get_barrier_semaphore()
    for d in peers():
        pl.semaphore_signal(barrier, inc=1, device_id={"dp": d}, device_id_type=pl.DeviceIdType.MESH)
    for t in tp_peers:
        pl.semaphore_signal(barrier, inc=1, device_id={"tp": t}, device_id_type=pl.DeviceIdType.MESH)
    with jax.named_scope("entry"):
        pl.semaphore_wait(barrier, 22)

    def mom_(r):
        for d in peers():
            send(mom.at[d, pl.ds(r * RC, RC), :], mom_x.at[r, me], "mom", "mom", r, dp=d)

    def dd(r):
        for s in range(4):
            send(grad.at[slots[s] * 2 + 1 - core, :, pl.ds(r * RC, RC), :], sib_g.at[s, r], "dd", "dd1" if s else "dd0",
                 r, dp=sib)

    lo, hi = pl.ds(0, 4), pl.ds(4, 4)

    def far(r):
        drain(local_sems.at[r], own_g.at[:, r])
        arrived(sib_g.at[0, r], "dd0", r)
        own_g[0, r] = own_g[0, r] + sib_g[0, r]
        send(own_g.at[0, r, lo], p2a.at[r], "rs", "p2", r, dp=dp_xp)
        send(own_g.at[0, r, hi], m2b.at[r], "rs", "p2", r, dp=dp_xm)

    def near(r):
        arrived(sib_g.at[pl.ds(1, 3), r], "dd1", r)
        own_g[1, r] = own_g[1, r] + sib_g[1, r]
        send(own_g.at[1, r, hi], p1b.at[r], "rs", "p1", r, dp=dp_xp)
        own_g[2, r] = own_g[2, r] + sib_g[2, r]
        send(own_g.at[2, r, lo], m1a.at[r], "rs", "p1", r, dp=dp_xm)

    def sum_(r):
        arrived(own_g.at[0, r], "p2", r)
        own_g[1, r, lo] = own_g[1, r, lo] + p2a[r]
        send(own_g.at[1, r, lo], p1a.at[r], "rs", "p1", r, dp=dp_xp)
        own_g[2, r, hi] = own_g[2, r, hi] + m2b[r]
        send(own_g.at[2, r, hi], m1b.at[r], "rs", "p1", r, dp=dp_xm)

    started = []

    def gather1(r):
        if not started:
            drain(local_sems.at[NC], mom_x.at[:, 0])
            sq_own[...] = jnp.zeros_like(sq_own)
        started.append(r)
        arrived(own_g.at[pl.ds(0, 2), r], "p1", r)
        arrived(mom_x.at[r, pl.ds(0, 7)], "mom", r)
        for half, (near_ref, far_ref) in enumerate(((m1a, p1a), (p1b, m1b))):
            ds = pl.ds(half * 4, 4)
            total = (own_g[3, r, ds] + sib_g[3, r, ds]) + (near_ref[r] + far_ref[r])
            mean = total * (1.0 / 8.0)
            mom_new = MOMENTUM * mom_x[r, ds] + mean
            mom_y[ds, pl.ds(r * RC, RC)] = mom_new
            upd = (mean + MOMENTUM * mom_new).astype(BF16)
            gath[z, y, r, ds] = upd
            upd = upd.astype(F32)
            sq_own[...] += jnp.sum((upd * upd).reshape(RC // 2, 8, 128), axis=0)
        for near_first in ((tp_zp, tp_yp), (tp_zm, tp_ym), (tp_z2, tp_y2)):
            send(gath.at[z, y, r, lo], gath.at[z, y, r, lo], "g1", "g1", r, tp=near_first[0])
            send(gath.at[z, y, r, hi], gath.at[z, y, r, hi], "g1", "g1", r, tp=near_first[1])
        if len(started) == NC:
            for t in tp_peers:
                send(sq_own, sq_all.at[tp], "sq", "sq", tp=t)

    def gather2(r):
        arrived(gath.at[0, pl.ds(0, 3), r], "g1", r)
        for t in (tp_yp, tp_ym):
            send(gath.at[:, y, r, lo], gath.at[:, y, r, lo], "g2", "g2", r, tp=t)
        for t in (tp_zp, tp_zm):
            send(gath.at[z, :, r, hi], gath.at[z, :, r, hi], "g2", "g2", r, tp=t)

    def forward2(r):
        arrived(gath.at[pl.ds(0, 2), :, r], "g2", r)
        for block, t in ((gath.at[:, ym, r, pl.ds(0, 2)], tp_yp), (gath.at[:, yp, r, pl.ds(2, 2)], tp_ym),
                         (gath.at[zm, :, r, pl.ds(4, 2)], tp_zp), (gath.at[zp, :, r, pl.ds(6, 2)], tp_zm)):
            send(block, block, "f2", "f2", r, tp=t)

    inv = []

    def norm(_):
        sq_all[tp] = sq_own[...]
        arrived(sq_all.at[pl.ds(0, 15)], "sq")
        total = jnp.sum(jnp.sum(sq_all[...], axis=0), keepdims=True)
        inv.append(1.0 / (jnp.sqrt(total) + NORM_EPS))

    def scale(r):
        arrived(gath.at[0, :, r], "f2", r)
        for i in range(4):
            for j in range(4):
                block = gath[i, j, r].reshape(CR, 128).astype(F32) * inv[0]
                x_cur[pl.ds(r * CR, CR), pl.ds(i * 512 + j * 128, 128)] = block.astype(BF16)

    def mirror_store(dst, block, first):
        dst[pl.ds(0, first + 256), pl.ds(first, 256)] = block
        if first:
            dst[pl.ds(first, 256), pl.ds(0, first)] = block[:first, :].T

    def gram_(i):
        first = i * 256
        mirror_store(gram, dot_nt(x_cur[pl.ds(0, first + 256), :], x_cur[pl.ds(first, 256), :]).astype(BF16), first)

    stages = {"mom": mom_, "dd": dd, "far": far, "near": near, "sum": sum_, "gather1": gather1, "gather2": gather2,
              "forward2": forward2, "norm": norm, "scale": scale, "gram": gram_}
    for name, r in ORDER:
        with jax.named_scope(f"{name}_{r}"):
            stages[name](r)

    w_own = pltpu.make_async_copy(weight, w_full.at[:, me], local_sems.at[NC + 1])
    w_own.start()
    for d in (dp_xp, dp_xm, dp_x2):
        send(weight, w_full.at[:, me], "w3", "w3", dp=d)
    send(weight, w_full.at[:, me], "w4", "w4", dp=sib)

    for d in peers():
        send(mom_y.at[d], mom_r.at[me], "back", "back", dp=d)

    def polynomial():
        for first in range(0, ROWS, 256):
            above, cols = pl.ds(0, first + 256), pl.ds(first, 256)
            square = dot_nn(gram[above, :], gram[:, cols])
            mirror_store(poly, (COEF_B * gram[above, cols].astype(F32) + COEF_C * square).astype(BF16), first)

    @pl.loop(0, NS_STEPS - 1)
    def _(step):
        polynomial()
        for first in range(0, COLS, 256):
            cols = pl.ds(first, 256)
            block = x_cur[:, cols]
            prod = dot_nn(poly[...], block)
            x_cur[:, cols] = (COEF_A * block.astype(F32) + prod).astype(BF16)
        for i in range(4):
            gram_(i)

    arrived(w_full.at[:, pl.ds(0, 3)], "w3")
    for d in (dp_xm, dp_xp, dp_x2):
        send(w_full.at[:, d], w_full.at[:, d], "w4", "w4", dp=sib)

    polynomial()
    own_cols = pl.ds(pl.multiple_of(tp * 128, 128), 128)
    block = x_cur[:, own_cols]

    def last(group, src, **device):
        send(src, src, "last", group, **device)

    final = (COEF_A * block.astype(F32) + dot_nn(poly[...], block)).astype(BF16)
    for r in range(NC):
        for d in range(8):
            x_full[me, pl.ds(d * 128 + r * RC, RC)] = final[r * CR + d * RC:r * CR + (d + 1) * RC]
    top, bot = pl.ds(0, 512), pl.ds(512, 512)
    last("fa", x_full.at[me, top], dp=dp_xp)
    last("fa", x_full.at[me, bot], dp=dp_xm)
    last("fb", x_full.at[me, bot], dp=dp_xp)
    last("fb", x_full.at[me, top], dp=dp_xm)
    last("fs", x_full.at[me], dp=sib)

    w_own.wait()
    arrived(w_full.at[:, pl.ds(0, 4)], "w4")

    def finish(mat):
        lr = rate[mat]
        dec = decay[0]
        wf = w_full[mat].reshape(ROWS, 128)
        new = wf - lr * (OUT_SCALE * x_full[mat].astype(F32) + dec * wf)
        full_out[mat] = new.astype(BF16)
        wo = w_full[mat, me]
        rows = pl.ds(pl.multiple_of(me * 128, 128), 128)
        weight_out[mat] = wo - lr * (OUT_SCALE * x_full[mat, rows].astype(F32) + dec * wo)

    mom_r[me] = mom_y[me]
    arrived(mom_r.at[pl.ds(0, 7)], "back")
    mom_out[...] = mom_r[...]

    pair = x_full.at[0]
    finish(me)
    arrived(pair, "fa")
    last("q", x_full.at[dp_xm, top], dp=dp_xp)
    last("q", x_full.at[dp_xp, bot], dp=dp_xm)
    arrived(pair, "fs")
    finish(sib)
    arrived(pair, "fb")
    last("s1", x_full.at[dp_xm], dp=sib)
    last("s1", x_full.at[dp_xp], dp=sib)
    finish(dp_xm)
    finish(dp_xp)
    arrived(x_full.at[pl.ds(0, 2)], "s1")
    finish(xm * 2 + 1 - core)
    finish(xp * 2 + 1 - core)
    arrived(pair, "q")
    last("s2", x_full.at[dp_x2, top], dp=sib)
    last("s2", x_full.at[dp_x2, bot], dp=sib)
    finish(dp_x2)
    arrived(pair, "s2")
    finish(x2 * 2 + 1 - core)

    with jax.named_scope("sends"):
        for group, like in (("dd", own_g), ("rs", own_g.at[pl.ds(0, 3)]), ("mom", mom_x.at[:, pl.ds(0, 7)]),
                            ("back", mom_r.at[pl.ds(0, 7)]), ("sq", sq_all.at[pl.ds(0, 15)]), ("g1", gath.at[0, pl.ds(0, 3)]), ("g2", gath.at[pl.ds(0, 2)]), ("f2", gath.at[0]),
                            ("w3", w_full.at[:, pl.ds(0, 3)]), ("w4", w_full.at[:, pl.ds(0, 4)]),
                            ("last", x_full.at[pl.ds(0, 7)])):
            drain(send_sems.at[SEND_GROUPS.index(group)], like)


def solution(mesh):
    def local_step(grad_local, mom_local, weight_local, learn_rate, decay_rate):
        hbm = pl.BlockSpec(memory_space=pltpu.HBM)
        vmem = pl.BlockSpec(memory_space=pltpu.VMEM)
        smem = pl.BlockSpec(memory_space=pltpu.SMEM)
        V = pltpu.VMEM
        return pl.pallas_call(
            muon_kernel,
            out_shape=(
                V((8, 128, 128), F32),
                V((8, 128, 128), F32),
                V((8, 1024, 128), BF16),
            ),
            in_specs=[hbm, hbm, hbm, smem, smem],
            out_specs=(vmem, vmem, vmem),
            scratch_shapes=[
                V((4, NC, 8, RC, 128), F32), V((4, NC, 8, RC, 128), F32),
                V((NC, 4, RC, 128), F32), V((NC, 4, RC, 128), F32), V((NC, 4, RC, 128), F32),
                V((NC, 4, RC, 128), F32), V((NC, 4, RC, 128), F32), V((NC, 4, RC, 128), F32),
                V((NC, 8, RC, 128), F32), V((8, 128, 128), F32), V((8, 128, 128), F32),
                V((4, 4, NC, 8, RC, 128), BF16), V((8, 128), F32), V((16, 8, 128), F32),
                V((ROWS, COLS), BF16), V((ROWS, ROWS), BF16), V((ROWS, ROWS), BF16),
                V((8, 8, 128, 128), F32), V((8, ROWS, 128), BF16),
                pltpu.SemaphoreType.DMA((len(SEND_GROUPS),)), pltpu.SemaphoreType.DMA((N_RECV,)),
                pltpu.SemaphoreType.DMA((N_LOCAL,)),
            ],
            compiler_params=pltpu.CompilerParams(
                collective_id=0, has_side_effects=True, vmem_limit_bytes=63_400_000),
            name="muon_step",
        )(grad_local.reshape(8, 8, 128, 128), mom_local, weight_local, learn_rate, decay_rate.reshape(1))

    return jax.shard_map(
        local_step,
        mesh=mesh,
        in_specs=(P(("rep", "dp"), None, None, "tp"), P("rep", "dp", "tp"), P("rep", "dp", "tp"), P("rep"), P()),
        out_specs=(P("rep", "dp", "tp"), P("rep", "dp", "tp"), P("rep", None, "tp")),
        check_vma=False,
    )
```

```python
import math
import jax
import jax.numpy as jnp
from jax import lax
from jax.experimental import pallas as pl
from jax.experimental.pallas import tpu as pltpu
from jax.sharding import PartitionSpec as P

MOMENTUM = 0.95
NS_STEPS = 5
COEF_A = 3.4445
COEF_B = -4.7750
COEF_C = 2.0315
NORM_EPS = 1e-7
F32 = jnp.float32
BF16 = jnp.bfloat16

MATS, ROWS, COLS = 8, 1024, 2048
NC = 8
RC = 128 // NC
CR = 8 * RC
OUT_SCALE = 0.2 * math.sqrt(max(ROWS, COLS))


def dot_nt(lhs, rhs):
    return lax.dot_general(lhs, rhs, (((1,), (1,)), ((), ())), preferred_element_type=F32)


def dot_nn(lhs, rhs):
    return lax.dot_general(lhs, rhs, (((1,), (0,)), ((), ())), preferred_element_type=F32)


ORDER = (
    ("mom", 1), ("dd", 0), ("dd", 1), ("far", 0), ("far", 1), ("dd", 4), ("mom", 0), ("mom", 4), ("dd", 7),
    ("near", 0), ("dd", 5), ("dd", 3), ("near", 1), ("far", 3), ("dd", 6), ("sum", 1), ("sum", 0), ("mom", 2),
    ("dd", 2), ("far", 5), ("mom", 3), ("far", 6), ("gather1", 1), ("far", 2), ("far", 4), ("gather1", 0),
    ("near", 3), ("sum", 3), ("mom", 6), ("near", 2), ("gather2", 1), ("sum", 2), ("near", 4), ("mom", 7), ("sum", 4),
    ("gather2", 0), ("gather1", 3), ("far", 7), ("near", 7), ("near", 6), ("near", 5), ("mom", 5), ("gather1", 2),
    ("forward2", 1), ("sum", 6), ("gather1", 4), ("sum", 7), ("forward2", 0), ("gather2", 3), ("sum", 5),
    ("gather2", 2), ("gather1", 6), ("gather1", 7), ("gather1", 5), ("forward2", 3), ("gather2", 4), ("gather2", 6),
    ("gather2", 5), ("sums", 0), ("gather2", 7), ("forward2", 2), ("forward2", 4), ("forward2", 5), ("forward2", 6),
    ("norm", 0), ("forward2", 7), ("scale", 0), ("scale", 3), ("scale", 1), ("scale", 2), ("gram", 0), ("gram", 1),
    ("scale", 4), ("scale", 5), ("gram", 2), ("scale", 6), ("scale", 7), ("gram", 3),
)

CHUNK_GROUPS = ("dd0", "dd1", "p2", "p1", "mom", "g1", "g2", "f2")
LATE_GROUPS = ("sqz", "sqy", "back", "w3", "w4", "fa", "fb", "fs", "s1", "q", "s2")
SEND_GROUPS = ("dd", "rs", "mom", "back", "sq", "g1", "g2", "w3", "w4", "last")
N_RECV = NC * len(CHUNK_GROUPS) + len(LATE_GROUPS)
N_LOCAL = NC + 2


def muon_kernel(grad, mom, weight, rate, decay, mom_out, weight_out, full_out,
                own_g, sib_g, p2a, p1b, p1a, m2b, m1a, m1b, mom_x, mom_y, mom_r, gath, sq_own, sq_z, sq_y,
                x_cur, gram, poly, w_full, x_full, send_sems, recv_sems, local_sems):
    me = lax.axis_index("dp")
    tp = lax.axis_index("tp")
    x, core = lax.div(me, 2), lax.rem(me, 2)
    z, y = lax.div(tp, 4), lax.rem(tp, 4)
    xp, xm, x2 = lax.rem(x + 1, 4), lax.rem(x + 3, 4), lax.rem(x + 2, 4)
    yp, ym, y2 = lax.rem(y + 1, 4), lax.rem(y + 3, 4), lax.rem(y + 2, 4)
    zp, zm, z2 = lax.rem(z + 1, 4), lax.rem(z + 3, 4), lax.rem(z + 2, 4)
    sib = x * 2 + 1 - core
    dp_xp, dp_xm, dp_x2 = xp * 2 + core, xm * 2 + core, x2 * 2 + core
    tp_yp, tp_ym, tp_y2 = z * 4 + yp, z * 4 + ym, z * 4 + y2
    tp_zp, tp_zm, tp_z2 = zp * 4 + y, zm * 4 + y, z2 * 4 + y
    slots = (x2, xp, xm, x)

    def recv_sem(group, r=None):
        if r is None:
            return recv_sems.at[NC * len(CHUNK_GROUPS) + LATE_GROUPS.index(group)]
        return recv_sems.at[r * len(CHUNK_GROUPS) + CHUNK_GROUPS.index(group)]

    def send(src, dst, sent, group, r=None, **device):
        pltpu.make_async_remote_copy(
            src_ref=src, dst_ref=dst, send_sem=send_sems.at[SEND_GROUPS.index(sent)], recv_sem=recv_sem(group, r),
            device_id=device, device_id_type=pl.DeviceIdType.MESH,
        ).start()

    def drain(sem, like):
        pltpu.make_async_copy(like, like, sem).wait()

    def arrived(like, group, r=None):
        drain(recv_sem(group, r), like)

    def peers(rest=7):
        return [lax.rem(me + i, 8) for i in range(1, rest + 1)]

    barrier = pltpu.get_barrier_semaphore()
    for d in peers():
        pl.semaphore_signal(barrier, inc=1, device_id={"dp": d}, device_id_type=pl.DeviceIdType.MESH)
    for t in (tp_yp, tp_ym, tp_y2, tp_zp, tp_zm, tp_z2):
        pl.semaphore_signal(barrier, inc=1, device_id={"tp": t}, device_id_type=pl.DeviceIdType.MESH)
    for r in range(NC):
        for s in range(4):
            pltpu.make_async_copy(grad.at[slots[s] * 2 + core, :, pl.ds(r * RC, RC), :], own_g.at[s, r],
                                  local_sems.at[r]).start()
        pltpu.make_async_copy(mom.at[me, pl.ds(r * RC, RC), :], mom_x.at[r, me], local_sems.at[NC]).start()

    with jax.named_scope("entry"):
        pl.semaphore_wait(barrier, 13)

    def mom_(r):
        for d in peers():
            send(mom.at[d, pl.ds(r * RC, RC), :], mom_x.at[r, me], "mom", "mom", r, dp=d)

    def dd(r):
        for s in range(4):
            send(grad.at[slots[s] * 2 + 1 - core, :, pl.ds(r * RC, RC), :], sib_g.at[s, r], "dd", "dd1" if s else "dd0",
                 r, dp=sib)

    lo, hi = pl.ds(0, 4), pl.ds(4, 4)

    def far(r):
        drain(local_sems.at[r], own_g.at[:, r])
        arrived(sib_g.at[0, r], "dd0", r)
        own_g[0, r] = own_g[0, r] + sib_g[0, r]
        send(own_g.at[0, r, lo], p2a.at[r], "rs", "p2", r, dp=dp_xp)
        send(own_g.at[0, r, hi], m2b.at[r], "rs", "p2", r, dp=dp_xm)

    def near(r):
        arrived(sib_g.at[pl.ds(1, 3), r], "dd1", r)
        own_g[1, r] = own_g[1, r] + sib_g[1, r]
        send(own_g.at[1, r, hi], p1b.at[r], "rs", "p1", r, dp=dp_xp)
        own_g[2, r] = own_g[2, r] + sib_g[2, r]
        send(own_g.at[2, r, lo], m1a.at[r], "rs", "p1", r, dp=dp_xm)

    def sum_(r):
        arrived(own_g.at[0, r], "p2", r)
        own_g[1, r, lo] = own_g[1, r, lo] + p2a[r]
        send(own_g.at[1, r, lo], p1a.at[r], "rs", "p1", r, dp=dp_xp)
        own_g[2, r, hi] = own_g[2, r, hi] + m2b[r]
        send(own_g.at[2, r, hi], m1b.at[r], "rs", "p1", r, dp=dp_xm)

    started = []

    def gather1(r):
        if not started:
            drain(local_sems.at[NC], mom_x.at[:, 0])
            sq_own[...] = jnp.zeros_like(sq_own)
        started.append(r)
        arrived(own_g.at[pl.ds(0, 2), r], "p1", r)
        arrived(mom_x.at[r, pl.ds(0, 7)], "mom", r)
        for half, (near_ref, far_ref) in enumerate(((m1a, p1a), (p1b, m1b))):
            ds = pl.ds(half * 4, 4)
            total = (own_g[3, r, ds] + sib_g[3, r, ds]) + (near_ref[r] + far_ref[r])
            mean = total * (1.0 / 8.0)
            mom_new = MOMENTUM * mom_x[r, ds] + mean
            mom_y[ds, pl.ds(r * RC, RC)] = mom_new
            upd = (mean + MOMENTUM * mom_new).astype(BF16)
            gath[z, y, r, ds] = upd
            upd = upd.astype(F32)
            sq_own[...] += jnp.sum((upd * upd).reshape(RC // 2, 8, 128), axis=0)
        for near_first in ((tp_zp, tp_yp), (tp_zm, tp_ym), (tp_z2, tp_y2)):
            send(gath.at[z, y, r, lo], gath.at[z, y, r, lo], "g1", "g1", r, tp=near_first[0])
            send(gath.at[z, y, r, hi], gath.at[z, y, r, hi], "g1", "g1", r, tp=near_first[1])
        if len(started) == NC:
            for t in (tp_zp, tp_zm, tp_z2):
                send(sq_own, sq_z.at[z], "sq", "sqz", tp=t)

    def gather2(r):
        arrived(gath.at[0, pl.ds(0, 3), r], "g1", r)
        for t in (tp_yp, tp_ym):
            send(gath.at[:, y, r, lo], gath.at[:, y, r, lo], "g2", "g2", r, tp=t)
        for t in (tp_zp, tp_zm):
            send(gath.at[z, :, r, hi], gath.at[z, :, r, hi], "g2", "g2", r, tp=t)

    def forward2(r):
        arrived(gath.at[pl.ds(0, 2), :, r], "g2", r)
        for block, t in ((gath.at[:, ym, r, pl.ds(0, 2)], tp_yp), (gath.at[:, yp, r, pl.ds(2, 2)], tp_ym),
                         (gath.at[zm, :, r, pl.ds(4, 2)], tp_zp), (gath.at[zp, :, r, pl.ds(6, 2)], tp_zm)):
            send(block, block, "g2", "f2", r, tp=t)

    inv = []

    def sums(_):
        sq_z[z] = sq_own[...]
        arrived(sq_z.at[pl.ds(0, 3)], "sqz")
        sq_y[y] = jnp.sum(sq_z[...], axis=0)
        for t in (tp_yp, tp_ym, tp_y2):
            send(sq_y.at[y], sq_y.at[y], "sq", "sqy", tp=t)

    def norm(_):
        arrived(sq_y.at[pl.ds(0, 3)], "sqy")
        total = jnp.sum(jnp.sum(sq_y[...], axis=0), keepdims=True)
        inv.append(1.0 / (jnp.sqrt(total) + NORM_EPS))

    def scale(r):
        arrived(gath.at[0, :, r], "f2", r)
        for i in range(4):
            for j in range(4):
                block = gath[i, j, r].reshape(CR, 128).astype(F32) * inv[0]
                x_cur[pl.ds(r * CR, CR), pl.ds(i * 512 + j * 128, 128)] = block.astype(BF16)

    def gram_rows(i):
        rows, left = pl.ds(i * 256, 256), pl.ds(0, i * 256)
        block = dot_nt(x_cur[rows, :], x_cur[pl.ds(0, i * 256 + 256), :]).astype(BF16)
        gram[rows, pl.ds(0, i * 256 + 256)] = block
        if i:
            gram[left, rows] = block[:, :i * 256].T

    def mirror_store(dst, block, first):
        dst[pl.ds(first, ROWS - first), pl.ds(first, 256)] = block
        if first + 256 < ROWS:
            dst[pl.ds(first, 256), pl.ds(first + 256, ROWS - first - 256)] = block[256:, :].T

    stages = {"mom": mom_, "dd": dd, "far": far, "near": near, "sum": sum_, "gather1": gather1, "gather2": gather2,
              "forward2": forward2, "norm": norm, "scale": scale, "sums": sums, "gram": gram_rows}
    for name, r in ORDER:
        with jax.named_scope(f"{name}_{r}"):
            stages[name](r)

    w_own = pltpu.make_async_copy(weight, w_full.at[:, me], local_sems.at[NC + 1])
    w_own.start()
    for d in (dp_xp, dp_xm, dp_x2):
        send(weight, w_full.at[:, me], "w3", "w3", dp=d)
    send(weight, w_full.at[:, me], "w4", "w4", dp=sib)

    for d in peers():
        send(mom_y.at[d], mom_r.at[me], "back", "back", dp=d)

    def polynomial():
        for first in range(0, ROWS, 256):
            below, cols = pl.ds(first, ROWS - first), pl.ds(first, 256)
            square = dot_nn(gram[below, :], gram[:, cols])
            mirror_store(poly, (COEF_B * gram[below, cols].astype(F32) + COEF_C * square).astype(BF16), first)

    @pl.loop(0, NS_STEPS - 1)
    def _(step):
        polynomial()
        for first in range(0, COLS, 256):
            cols = pl.ds(first, 256)
            block = x_cur[:, cols]
            prod = dot_nn(poly[...], block)
            x_cur[:, cols] = (COEF_A * block.astype(F32) + prod).astype(BF16)
        for first in range(0, ROWS, 256):
            below = pl.ds(first, ROWS - first)
            mirror_store(gram, dot_nt(x_cur[below, :], x_cur[pl.ds(first, 256), :]).astype(BF16), first)

    arrived(w_full.at[:, pl.ds(0, 3)], "w3")
    for d in (dp_xm, dp_xp, dp_x2):
        send(w_full.at[:, d], w_full.at[:, d], "w4", "w4", dp=sib)

    polynomial()
    own_cols = pl.ds(pl.multiple_of(tp * 128, 128), 128)
    block = x_cur[:, own_cols]

    def last(group, src, **device):
        send(src, src, "last", group, **device)

    final = (COEF_A * block.astype(F32) + dot_nn(poly[...], block)).astype(BF16)
    for r in range(NC):
        for d in range(8):
            x_full[me, pl.ds(d * 128 + r * RC, RC)] = final[r * CR + d * RC:r * CR + (d + 1) * RC]
    top, bot = pl.ds(0, 512), pl.ds(512, 512)
    last("fa", x_full.at[me, top], dp=dp_xp)
    last("fa", x_full.at[me, bot], dp=dp_xm)
    last("fb", x_full.at[me, bot], dp=dp_xp)
    last("fb", x_full.at[me, top], dp=dp_xm)
    last("fs", x_full.at[me], dp=sib)

    w_own.wait()
    arrived(w_full.at[:, pl.ds(0, 4)], "w4")

    def sent(*pairs):
        for group, like in pairs:
            drain(send_sems.at[SEND_GROUPS.index(group)], like)

    def finish(mat):
        lr = rate[mat]
        dec = decay[0]
        wf = w_full[mat].reshape(ROWS, 128)
        new = wf - lr * (OUT_SCALE * x_full[mat].astype(F32) + dec * wf)
        full_out[mat] = new.astype(BF16)
        wo = w_full[mat, me]
        rows = pl.ds(pl.multiple_of(me * 128, 128), 128)
        weight_out[mat] = wo - lr * (OUT_SCALE * x_full[mat, rows].astype(F32) + dec * wo)

    mom_r[me] = mom_y[me]
    arrived(mom_r.at[pl.ds(0, 7)], "back")
    mom_out[...] = mom_r[...]

    pair = x_full.at[0]
    finish(me)
    sent(("dd", own_g), ("rs", own_g.at[pl.ds(0, 3)]), ("mom", mom_x.at[:, pl.ds(0, 7)]),
         ("back", mom_r.at[pl.ds(0, 7)]), ("sq", mom_r.at[0, pl.ds(0, 48)]), ("g1", gath.at[0, pl.ds(0, 3)]),
         ("g2", gath.at[pl.ds(0, 3)]), ("w3", w_full.at[:, pl.ds(0, 3)]), ("w4", w_full.at[:, pl.ds(0, 4)]))
    arrived(pair, "fa")
    last("q", x_full.at[dp_xm, top], dp=dp_xp)
    last("q", x_full.at[dp_xp, bot], dp=dp_xm)
    arrived(pair, "fs")
    finish(sib)
    arrived(pair, "fb")
    last("s1", x_full.at[dp_xm], dp=sib)
    last("s1", x_full.at[dp_xp], dp=sib)
    finish(dp_xm)
    finish(dp_xp)
    arrived(x_full.at[pl.ds(0, 2)], "s1")
    finish(xm * 2 + 1 - core)
    finish(xp * 2 + 1 - core)
    arrived(pair, "q")
    last("s2", x_full.at[dp_x2, top], dp=sib)
    last("s2", x_full.at[dp_x2, bot], dp=sib)
    finish(dp_x2)
    arrived(pair, "s2")
    finish(x2 * 2 + 1 - core)

    sent(("last", x_full.at[pl.ds(0, 7)]))


def solution(mesh):
    def local_step(grad_local, mom_local, weight_local, learn_rate, decay_rate):
        hbm = pl.BlockSpec(memory_space=pltpu.HBM)
        vmem = pl.BlockSpec(memory_space=pltpu.VMEM)
        smem = pl.BlockSpec(memory_space=pltpu.SMEM)
        V = pltpu.VMEM
        return pl.pallas_call(
            muon_kernel,
            out_shape=(
                V((8, 128, 128), F32),
                V((8, 128, 128), F32),
                V((8, 1024, 128), BF16),
            ),
            in_specs=[hbm, hbm, hbm, smem, smem],
            out_specs=(vmem, vmem, vmem),
            scratch_shapes=[
                V((4, NC, 8, RC, 128), F32), V((4, NC, 8, RC, 128), F32),
                V((NC, 4, RC, 128), F32), V((NC, 4, RC, 128), F32), V((NC, 4, RC, 128), F32),
                V((NC, 4, RC, 128), F32), V((NC, 4, RC, 128), F32), V((NC, 4, RC, 128), F32),
                V((NC, 8, RC, 128), F32), V((8, 128, 128), F32), V((8, 128, 128), F32),
                V((4, 4, NC, 8, RC, 128), BF16), V((8, 128), F32), V((4, 8, 128), F32), V((4, 8, 128), F32),
                V((ROWS, COLS), BF16), V((ROWS, ROWS), BF16), V((ROWS, ROWS), BF16),
                V((8, 8, 128, 128), F32), V((8, ROWS, 128), BF16),
                pltpu.SemaphoreType.DMA((len(SEND_GROUPS),)), pltpu.SemaphoreType.DMA((N_RECV,)),
                pltpu.SemaphoreType.DMA((N_LOCAL,)),
            ],
            compiler_params=pltpu.CompilerParams(
                collective_id=0, has_side_effects=True, vmem_limit_bytes=63_400_000),
            name="muon_step",
        )(grad_local.reshape(8, 8, 128, 128), mom_local, weight_local, learn_rate, decay_rate.reshape(1))

    return jax.shard_map(
        local_step,
        mesh=mesh,
        in_specs=(P(("rep", "dp"), None, None, "tp"), P("rep", "dp", "tp"), P("rep", "dp", "tp"), P("rep"), P()),
        out_specs=(P("rep", "dp", "tp"), P("rep", "dp", "tp"), P("rep", None, "tp")),
        check_vma=False,
    )
```

```python
import math
import jax
import jax.numpy as jnp
from jax import lax
from jax.experimental import pallas as pl
from jax.experimental.pallas import tpu as pltpu
from jax.sharding import PartitionSpec as P

MOMENTUM = 0.95
NS_STEPS = 5
COEF_A = 3.4445
COEF_B = -4.7750
COEF_C = 2.0315
NORM_EPS = 1e-7
F32 = jnp.float32
BF16 = jnp.bfloat16

MATS, ROWS, COLS = 8, 1024, 2048
NC = 8
RC = 128 // NC
CR = 8 * RC
MIX = MOMENTUM * MOMENTUM / (1.0 + MOMENTUM)
OUT_SCALE = 0.2 * math.sqrt(max(ROWS, COLS))


def dot_nt(lhs, rhs):
    return lax.dot_general(lhs, rhs, (((1,), (1,)), ((), ())), preferred_element_type=F32)


def dot_nn(lhs, rhs):
    return lax.dot_general(lhs, rhs, (((1,), (0,)), ((), ())), preferred_element_type=F32)


ORDER = (
    ("dd", 0), ("dd", 4), ("dd", 6), ("far", 0), ("dd", 2), ("near", 0), ("dd", 3), ("dd", 1), ("far", 2), ("far", 1),
    ("near", 2), ("sum", 0), ("dd", 5), ("near", 1), ("far", 3), ("sum", 1), ("sum", 2), ("near", 3), ("gather1", 0),
    ("far", 4), ("dd", 7), ("sum", 3), ("far", 5), ("gather1", 1), ("near", 4), ("far", 6), ("gather1", 2),
    ("sum", 4), ("far", 7), ("gather2", 0), ("gather1", 3), ("near", 5), ("sum", 5), ("near", 7), ("gather2", 1),
    ("near", 6), ("sum", 6), ("gather2", 2), ("gather1", 4), ("sum", 7), ("forward2", 0), ("gather1", 5),
    ("gather2", 3), ("gather1", 6), ("gather1", 7), ("forward2", 1), ("gather2", 4), ("gather2", 5), ("forward2", 2),
    ("gather2", 6), ("sums", 0), ("gather2", 7), ("forward2", 3), ("forward2", 4), ("forward2", 5), ("forward2", 6),
    ("forward2", 7), ("norm", 0), ("scale", 2), ("scale", 1), ("scale", 0), ("scale", 3), ("gram", 0), ("gram", 1),
    ("scale", 4), ("scale", 5), ("gram", 2), ("scale", 6), ("scale", 7), ("gram", 3),
)

CHUNK_GROUPS = ("dd0", "dd1", "p2", "p1", "g1", "g2", "f2")
LATE_GROUPS = ("mom", "sqz", "sqy", "back", "w3", "w4", "fa", "fb", "fs", "s1", "q", "s2")
SEND_GROUPS = ("dd", "rs", "mom", "back", "sq", "g1", "g2", "w3", "w4", "last")
N_RECV = NC * len(CHUNK_GROUPS) + len(LATE_GROUPS)
N_LOCAL = NC + 2


def muon_kernel(grad, mom, weight, rate, decay, mom_out, weight_out, full_out,
                own_g, sib_g, p2a, p1b, p1a, m2b, m1a, m1b, mom_s, mix, mom_r, gath, sq_own, sq_z, sq_y,
                x_cur, gram, poly, w_full, x_full, send_sems, recv_sems, local_sems):
    me = lax.axis_index("dp")
    tp = lax.axis_index("tp")
    x, core = lax.div(me, 2), lax.rem(me, 2)
    z, y = lax.div(tp, 4), lax.rem(tp, 4)
    xp, xm, x2 = lax.rem(x + 1, 4), lax.rem(x + 3, 4), lax.rem(x + 2, 4)
    yp, ym, y2 = lax.rem(y + 1, 4), lax.rem(y + 3, 4), lax.rem(y + 2, 4)
    zp, zm, z2 = lax.rem(z + 1, 4), lax.rem(z + 3, 4), lax.rem(z + 2, 4)
    sib = x * 2 + 1 - core
    dp_xp, dp_xm, dp_x2 = xp * 2 + core, xm * 2 + core, x2 * 2 + core
    tp_yp, tp_ym, tp_y2 = z * 4 + yp, z * 4 + ym, z * 4 + y2
    tp_zp, tp_zm, tp_z2 = zp * 4 + y, zm * 4 + y, z2 * 4 + y
    slots = (x2, xp, xm, x)

    def recv_sem(group, r=None):
        if r is None:
            return recv_sems.at[NC * len(CHUNK_GROUPS) + LATE_GROUPS.index(group)]
        return recv_sems.at[r * len(CHUNK_GROUPS) + CHUNK_GROUPS.index(group)]

    def send(src, dst, sent, group, r=None, **device):
        pltpu.make_async_remote_copy(
            src_ref=src, dst_ref=dst, send_sem=send_sems.at[SEND_GROUPS.index(sent)], recv_sem=recv_sem(group, r),
            device_id=device, device_id_type=pl.DeviceIdType.MESH,
        ).start()

    def drain(sem, like):
        pltpu.make_async_copy(like, like, sem).wait()

    def arrived(like, group, r=None):
        drain(recv_sem(group, r), like)

    def peers(rest=7):
        return [lax.rem(me + i, 8) for i in range(1, rest + 1)]

    barrier = pltpu.get_barrier_semaphore()
    for d in peers():
        pl.semaphore_signal(barrier, inc=1, device_id={"dp": d}, device_id_type=pl.DeviceIdType.MESH)
    for t in (tp_yp, tp_ym, tp_y2, tp_zp, tp_zm, tp_z2):
        pl.semaphore_signal(barrier, inc=1, device_id={"tp": t}, device_id_type=pl.DeviceIdType.MESH)
    for r in range(NC):
        for s in range(4):
            pltpu.make_async_copy(grad.at[slots[s] * 2 + core, :, pl.ds(r * RC, RC), :], own_g.at[s, r],
                                  local_sems.at[r]).start()
    mom_load = pltpu.make_async_copy(mom, mom_out, local_sems.at[NC])
    mom_load.start()

    with jax.named_scope("entry"):
        pl.semaphore_wait(barrier, 13)

    def dd(r):
        for s in range(4):
            send(grad.at[slots[s] * 2 + 1 - core, :, pl.ds(r * RC, RC), :], sib_g.at[s, r], "dd", "dd1" if s else "dd0",
                 r, dp=sib)
        if r == 0:
            for s in range(4):
                send(mom.at[slots[s] * 2 + 1 - core], mom_s.at[s], "mom", "mom", dp=sib)

    lo, hi = pl.ds(0, 4), pl.ds(4, 4)

    def chip_terms(s, r):
        rows = pl.ds(r * RC, RC)
        own_g[s, r] = (own_g[s, r] + sib_g[s, r]) * (1.0 / 8.0)
        own_g[s, r, me] = own_g[s, r, me] + MIX * mom_out[slots[s] * 2 + core, rows]
        own_g[s, r, sib] = own_g[s, r, sib] + MIX * mom_s[s, rows]

    def far(r):
        drain(local_sems.at[r], own_g.at[:, r])
        if r == 0:
            mom_load.wait()
            arrived(mom_s, "mom")
        arrived(sib_g.at[0, r], "dd0", r)
        chip_terms(0, r)
        send(own_g.at[0, r, lo], p2a.at[r], "rs", "p2", r, dp=dp_xp)
        send(own_g.at[0, r, hi], m2b.at[r], "rs", "p2", r, dp=dp_xm)

    def near(r):
        arrived(sib_g.at[pl.ds(1, 3), r], "dd1", r)
        chip_terms(1, r)
        send(own_g.at[1, r, hi], p1b.at[r], "rs", "p1", r, dp=dp_xp)
        chip_terms(2, r)
        send(own_g.at[2, r, lo], m1a.at[r], "rs", "p1", r, dp=dp_xm)

    def sum_(r):
        arrived(own_g.at[0, r], "p2", r)
        own_g[1, r, lo] = own_g[1, r, lo] + p2a[r]
        send(own_g.at[1, r, lo], p1a.at[r], "rs", "p1", r, dp=dp_xp)
        own_g[2, r, hi] = own_g[2, r, hi] + m2b[r]
        send(own_g.at[2, r, hi], m1b.at[r], "rs", "p1", r, dp=dp_xm)

    started = []

    def gather1(r):
        if not started:
            sq_own[...] = jnp.zeros_like(sq_own)
        started.append(r)
        arrived(own_g.at[pl.ds(0, 2), r], "p1", r)
        chip_terms(3, r)
        for half, (near_ref, far_ref) in enumerate(((m1a, p1a), (p1b, m1b))):
            ds = pl.ds(half * 4, 4)
            total = own_g[3, r, ds] + (near_ref[r] + far_ref[r])
            mix[ds, pl.ds(r * RC, RC)] = total
            upd = ((1.0 + MOMENTUM) * total).astype(BF16)
            gath[z, y, r, ds] = upd
            upd = upd.astype(F32)
            sq_own[...] += jnp.sum((upd * upd).reshape(RC // 2, 8, 128), axis=0)
        for near_first in ((tp_zp, tp_yp), (tp_zm, tp_ym), (tp_z2, tp_y2)):
            send(gath.at[z, y, r, lo], gath.at[z, y, r, lo], "g1", "g1", r, tp=near_first[0])
            send(gath.at[z, y, r, hi], gath.at[z, y, r, hi], "g1", "g1", r, tp=near_first[1])
        for t in (tp_yp, tp_ym):
            send(gath.at[z, y, r, lo], gath.at[z, y, r, lo], "g2", "g2", r, tp=t)
        for t in (tp_zp, tp_zm):
            send(gath.at[z, y, r, hi], gath.at[z, y, r, hi], "g2", "g2", r, tp=t)
        if len(started) == NC:
            for t in (tp_zp, tp_zm, tp_z2):
                send(sq_own, sq_z.at[z], "sq", "sqz", tp=t)

    def gather2(r):
        arrived(gath.at[0, pl.ds(0, 3), r], "g1", r)
        for other in (zp, zm, z2):
            for t in (tp_yp, tp_ym):
                send(gath.at[other, y, r, lo], gath.at[other, y, r, lo], "g2", "g2", r, tp=t)
        for other in (yp, ym, y2):
            for t in (tp_zp, tp_zm):
                send(gath.at[z, other, r, hi], gath.at[z, other, r, hi], "g2", "g2", r, tp=t)

    def forward2(r):
        arrived(gath.at[pl.ds(0, 2), :, r], "g2", r)
        for block, t in ((gath.at[:, ym, r, pl.ds(0, 2)], tp_yp), (gath.at[:, yp, r, pl.ds(2, 2)], tp_ym),
                         (gath.at[zm, :, r, pl.ds(4, 2)], tp_zp), (gath.at[zp, :, r, pl.ds(6, 2)], tp_zm)):
            send(block, block, "g2", "f2", r, tp=t)

    inv = []

    def sums(_):
        sq_z[z] = sq_own[...]
        arrived(sq_z.at[pl.ds(0, 3)], "sqz")
        sq_y[y] = jnp.sum(sq_z[...], axis=0)
        for t in (tp_yp, tp_ym, tp_y2):
            send(sq_y.at[y], sq_y.at[y], "sq", "sqy", tp=t)

    def norm(_):
        arrived(sq_y.at[pl.ds(0, 3)], "sqy")
        total = jnp.sum(jnp.sum(sq_y[...], axis=0), keepdims=True)
        inv.append(1.0 / (jnp.sqrt(total) + NORM_EPS))

    def scale(r):
        arrived(gath.at[0, :, r], "f2", r)
        for i in range(4):
            for j in range(4):
                block = gath[i, j, r].reshape(CR, 128).astype(F32) * inv[0]
                x_cur[pl.ds(r * CR, CR), pl.ds(i * 512 + j * 128, 128)] = block.astype(BF16)

    def gram_rows(i):
        rows, left = pl.ds(i * 256, 256), pl.ds(0, i * 256)
        block = dot_nt(x_cur[rows, :], x_cur[pl.ds(0, i * 256 + 256), :]).astype(BF16)
        gram[rows, pl.ds(0, i * 256 + 256)] = block
        if i:
            gram[left, rows] = block[:, :i * 256].T

    def mirror_store(dst, block, first):
        dst[pl.ds(first, ROWS - first), pl.ds(first, 256)] = block
        if first + 256 < ROWS:
            dst[pl.ds(first, 256), pl.ds(first + 256, ROWS - first - 256)] = block[256:, :].T

    stages = {"dd": dd, "far": far, "near": near, "sum": sum_, "gather1": gather1, "gather2": gather2,
              "forward2": forward2, "norm": norm, "scale": scale, "sums": sums, "gram": gram_rows}
    for name, r in ORDER:
        with jax.named_scope(f"{name}_{r}"):
            stages[name](r)

    w_own = pltpu.make_async_copy(weight, w_full.at[:, me], local_sems.at[NC + 1])
    w_own.start()
    for d in (dp_xp, dp_xm, dp_x2):
        send(weight, w_full.at[:, me], "w3", "w3", dp=d)
    send(weight, w_full.at[:, me], "w4", "w4", dp=sib)

    for d in peers():
        send(mix.at[d], mom_r.at[me], "back", "back", dp=d)

    def polynomial():
        for first in range(0, ROWS, 256):
            below, cols = pl.ds(first, ROWS - first), pl.ds(first, 256)
            square = dot_nn(gram[below, :], gram[:, cols])
            mirror_store(poly, (COEF_B * gram[below, cols].astype(F32) + COEF_C * square).astype(BF16), first)

    @pl.loop(0, NS_STEPS - 1)
    def _(step):
        polynomial()
        for first in range(0, COLS, 256):
            cols = pl.ds(first, 256)
            block = x_cur[:, cols]
            prod = dot_nn(poly[...], block)
            x_cur[:, cols] = (COEF_A * block.astype(F32) + prod).astype(BF16)
        for first in range(0, ROWS, 256):
            below = pl.ds(first, ROWS - first)
            mirror_store(gram, dot_nt(x_cur[below, :], x_cur[pl.ds(first, 256), :]).astype(BF16), first)

    arrived(w_full.at[:, pl.ds(0, 3)], "w3")
    for d in (dp_xm, dp_xp, dp_x2):
        send(w_full.at[:, d], w_full.at[:, d], "w4", "w4", dp=sib)

    polynomial()
    own_cols = pl.ds(pl.multiple_of(tp * 128, 128), 128)
    block = x_cur[:, own_cols]

    def last(group, src, **device):
        send(src, src, "last", group, **device)

    final = (COEF_A * block.astype(F32) + dot_nn(poly[...], block)).astype(BF16)
    for r in range(NC):
        for d in range(8):
            x_full[me, pl.ds(d * 128 + r * RC, RC)] = final[r * CR + d * RC:r * CR + (d + 1) * RC]
    top, bot = pl.ds(0, 512), pl.ds(512, 512)
    last("fa", x_full.at[me, top], dp=dp_xp)
    last("fa", x_full.at[me, bot], dp=dp_xm)
    last("fb", x_full.at[me, bot], dp=dp_xp)
    last("fb", x_full.at[me, top], dp=dp_xm)
    last("fs", x_full.at[me], dp=sib)

    w_own.wait()
    arrived(w_full.at[:, pl.ds(0, 4)], "w4")

    def sent(*pairs):
        for group, like in pairs:
            drain(send_sems.at[SEND_GROUPS.index(group)], like)

    def finish(mat):
        lr = rate[mat]
        dec = decay[0]
        wf = w_full[mat].reshape(ROWS, 128)
        new = wf - lr * (OUT_SCALE * x_full[mat].astype(F32) + dec * wf)
        full_out[mat] = new.astype(BF16)
        wo = w_full[mat, me]
        rows = pl.ds(pl.multiple_of(me * 128, 128), 128)
        weight_out[mat] = wo - lr * (OUT_SCALE * x_full[mat, rows].astype(F32) + dec * wo)

    mom_r[me] = mix[me]
    arrived(mom_r.at[pl.ds(0, 7)], "back")
    mom_out[...] = mom_r[...] + (MOMENTUM - MIX) * mom_out[...]

    pair = x_full.at[0]
    finish(me)
    sent(("dd", own_g), ("rs", own_g.at[pl.ds(0, 3)]), ("mom", mom_s),
         ("back", mom_r.at[pl.ds(0, 7)]), ("sq", mom_r.at[0, pl.ds(0, 48)]), ("g1", gath.at[0, pl.ds(0, 3)]),
         ("g2", gath.at[pl.ds(0, 3)]), ("w3", w_full.at[:, pl.ds(0, 3)]), ("w4", w_full.at[:, pl.ds(0, 4)]))
    arrived(pair, "fa")
    last("q", x_full.at[dp_xm, top], dp=dp_xp)
    last("q", x_full.at[dp_xp, bot], dp=dp_xm)
    arrived(pair, "fs")
    finish(sib)
    arrived(pair, "fb")
    last("s1", x_full.at[dp_xm], dp=sib)
    last("s1", x_full.at[dp_xp], dp=sib)
    finish(dp_xm)
    finish(dp_xp)
    arrived(x_full.at[pl.ds(0, 2)], "s1")
    finish(xm * 2 + 1 - core)
    finish(xp * 2 + 1 - core)
    arrived(pair, "q")
    last("s2", x_full.at[dp_x2, top], dp=sib)
    last("s2", x_full.at[dp_x2, bot], dp=sib)
    finish(dp_x2)
    arrived(pair, "s2")
    finish(x2 * 2 + 1 - core)

    sent(("last", x_full.at[pl.ds(0, 7)]))


def solution(mesh):
    def local_step(grad_local, mom_local, weight_local, learn_rate, decay_rate):
        hbm = pl.BlockSpec(memory_space=pltpu.HBM)
        vmem = pl.BlockSpec(memory_space=pltpu.VMEM)
        smem = pl.BlockSpec(memory_space=pltpu.SMEM)
        V = pltpu.VMEM
        return pl.pallas_call(
            muon_kernel,
            out_shape=(
                V((8, 128, 128), F32),
                V((8, 128, 128), F32),
                V((8, 1024, 128), BF16),
            ),
            in_specs=[hbm, hbm, hbm, smem, smem],
            out_specs=(vmem, vmem, vmem),
            scratch_shapes=[
                V((4, NC, 8, RC, 128), F32), V((4, NC, 8, RC, 128), F32),
                V((NC, 4, RC, 128), F32), V((NC, 4, RC, 128), F32), V((NC, 4, RC, 128), F32),
                V((NC, 4, RC, 128), F32), V((NC, 4, RC, 128), F32), V((NC, 4, RC, 128), F32),
                V((4, 128, 128), F32), V((8, 128, 128), F32), V((8, 128, 128), F32),
                V((4, 4, NC, 8, RC, 128), BF16), V((8, 128), F32), V((4, 8, 128), F32), V((4, 8, 128), F32),
                V((ROWS, COLS), BF16), V((ROWS, ROWS), BF16), V((ROWS, ROWS), BF16),
                V((8, 8, 128, 128), F32), V((8, ROWS, 128), BF16),
                pltpu.SemaphoreType.DMA((len(SEND_GROUPS),)), pltpu.SemaphoreType.DMA((N_RECV,)),
                pltpu.SemaphoreType.DMA((N_LOCAL,)),
            ],
            compiler_params=pltpu.CompilerParams(
                collective_id=0, has_side_effects=True, vmem_limit_bytes=63_400_000),
            name="muon_step",
        )(grad_local.reshape(8, 8, 128, 128), mom_local, weight_local, learn_rate, decay_rate.reshape(1))

    return jax.shard_map(
        local_step,
        mesh=mesh,
        in_specs=(P(("rep", "dp"), None, None, "tp"), P("rep", "dp", "tp"), P("rep", "dp", "tp"), P("rep"), P()),
        out_specs=(P("rep", "dp", "tp"), P("rep", "dp", "tp"), P("rep", None, "tp")),
        check_vma=False,
    )
```

```python
import math
import jax
import jax.numpy as jnp
from jax import lax
from jax.experimental import pallas as pl
from jax.experimental.pallas import tpu as pltpu
from jax.sharding import PartitionSpec as P

MOMENTUM = 0.95
NS_STEPS = 5
COEF_A = 3.4445
COEF_B = -4.7750
COEF_C = 2.0315
NORM_EPS = 1e-7
F32 = jnp.float32
BF16 = jnp.bfloat16

MATS, ROWS, COLS = 8, 1024, 2048
NC = 8
RC = 128 // NC
CR = 8 * RC
MIX = MOMENTUM * MOMENTUM / (1.0 + MOMENTUM)
OUT_SCALE = 0.2 * math.sqrt(max(ROWS, COLS))


def dot_nt(lhs, rhs):
    return lax.dot_general(lhs, rhs, (((1,), (1,)), ((), ())), preferred_element_type=F32)


def dot_nn(lhs, rhs):
    return lax.dot_general(lhs, rhs, (((1,), (0,)), ((), ())), preferred_element_type=F32)


ORDER = (
    ("dd", 0), ("dd", 4), ("dd", 6), ("far", 0), ("dd", 2), ("near", 0), ("dd", 3), ("dd", 1), ("far", 2), ("far", 1),
    ("near", 2), ("sum", 0), ("dd", 5), ("near", 1), ("far", 3), ("sum", 1), ("sum", 2), ("near", 3), ("gather1", 0),
    ("far", 4), ("dd", 7), ("sum", 3), ("far", 5), ("gather1", 1), ("near", 4), ("far", 6), ("gather1", 2),
    ("sum", 4), ("far", 7), ("gather2", 0), ("gather1", 3), ("near", 5), ("sum", 5), ("near", 7), ("gather2", 1),
    ("near", 6), ("sum", 6), ("gather2", 2), ("gather1", 4), ("sum", 7), ("forward2", 0), ("gather1", 5),
    ("gather2", 3), ("gather1", 6), ("gather1", 7), ("forward2", 1), ("gather2", 4), ("gather2", 5), ("forward2", 2),
    ("gather2", 6), ("sums", 0), ("gather2", 7), ("forward2", 3), ("forward2", 4), ("forward2", 5), ("forward2", 6),
    ("forward2", 7), ("norm", 0), ("scale", 2), ("scale", 1), ("scale", 0), ("scale", 3), ("gram", 0), ("gram", 1),
    ("scale", 4), ("scale", 5), ("gram", 2), ("scale", 6), ("scale", 7), ("gram", 3),
)

CHUNK_GROUPS = ("dd0", "dd1", "p2", "p1", "g1", "g2", "f2")
LATE_GROUPS = ("mom", "sqz", "sqy", "back", "w3", "w4", "fa", "fb", "fs", "s1", "q", "s2")
SEND_GROUPS = ("dd", "rs", "mom", "back", "sq", "g1", "g2", "w3", "w4", "last")
N_RECV = NC * len(CHUNK_GROUPS) + len(LATE_GROUPS)
N_LOCAL = NC + 2


def muon_kernel(grad, mom, weight, rate, decay, pair_out, full_out,
                own_g, sib_g, p2a, p1b, p1a, m2b, m1a, m1b, mom_v, mom_s, mix, mom_r, gath, sq_own, sq_z, sq_y,
                x_cur, gram, poly, w_full, x_full, send_sems, recv_sems, local_sems):
    me = lax.axis_index("dp")
    tp = lax.axis_index("tp")
    x, core = lax.div(me, 2), lax.rem(me, 2)
    z, y = lax.div(tp, 4), lax.rem(tp, 4)
    xp, xm, x2 = lax.rem(x + 1, 4), lax.rem(x + 3, 4), lax.rem(x + 2, 4)
    yp, ym, y2 = lax.rem(y + 1, 4), lax.rem(y + 3, 4), lax.rem(y + 2, 4)
    zp, zm, z2 = lax.rem(z + 1, 4), lax.rem(z + 3, 4), lax.rem(z + 2, 4)
    sib = x * 2 + 1 - core
    dp_xp, dp_xm, dp_x2 = xp * 2 + core, xm * 2 + core, x2 * 2 + core
    tp_yp, tp_ym, tp_y2 = z * 4 + yp, z * 4 + ym, z * 4 + y2
    tp_zp, tp_zm, tp_z2 = zp * 4 + y, zm * 4 + y, z2 * 4 + y
    slots = (x2, xp, xm, x)

    def recv_sem(group, r=None):
        if r is None:
            return recv_sems.at[NC * len(CHUNK_GROUPS) + LATE_GROUPS.index(group)]
        return recv_sems.at[r * len(CHUNK_GROUPS) + CHUNK_GROUPS.index(group)]

    def send(src, dst, sent, group, r=None, **device):
        pltpu.make_async_remote_copy(
            src_ref=src, dst_ref=dst, send_sem=send_sems.at[SEND_GROUPS.index(sent)], recv_sem=recv_sem(group, r),
            device_id=device, device_id_type=pl.DeviceIdType.MESH,
        ).start()

    def drain(sem, like):
        pltpu.make_async_copy(like, like, sem).wait()

    def arrived(like, group, r=None):
        drain(recv_sem(group, r), like)

    def peers(rest=7):
        return [lax.rem(me + i, 8) for i in range(1, rest + 1)]

    barrier = pltpu.get_barrier_semaphore()
    for d in peers():
        pl.semaphore_signal(barrier, inc=1, device_id={"dp": d}, device_id_type=pl.DeviceIdType.MESH)
    for t in (tp_yp, tp_ym, tp_y2, tp_zp, tp_zm, tp_z2):
        pl.semaphore_signal(barrier, inc=1, device_id={"tp": t}, device_id_type=pl.DeviceIdType.MESH)
    for r in range(NC):
        for s in range(4):
            pltpu.make_async_copy(grad.at[slots[s] * 2 + core, :, pl.ds(r * RC, RC), :], own_g.at[s, r],
                                  local_sems.at[r]).start()
    mom_load = pltpu.make_async_copy(mom, mom_v, local_sems.at[NC])
    mom_load.start()

    with jax.named_scope("entry"):
        pl.semaphore_wait(barrier, 13)

    def dd(r):
        for s in range(4):
            send(grad.at[slots[s] * 2 + 1 - core, :, pl.ds(r * RC, RC), :], sib_g.at[s, r], "dd", "dd1" if s else "dd0",
                 r, dp=sib)
        if r == 0:
            for s in range(4):
                send(mom.at[slots[s] * 2 + 1 - core], mom_s.at[s], "mom", "mom", dp=sib)

    lo, hi = pl.ds(0, 4), pl.ds(4, 4)

    def chip_terms(s, r):
        rows = pl.ds(r * RC, RC)
        own_g[s, r] = (own_g[s, r] + sib_g[s, r]) * (1.0 / 8.0)
        own_g[s, r, me] = own_g[s, r, me] + MIX * mom_v[slots[s] * 2 + core, rows]
        own_g[s, r, sib] = own_g[s, r, sib] + MIX * mom_s[s, rows]

    def far(r):
        drain(local_sems.at[r], own_g.at[:, r])
        if r == 0:
            mom_load.wait()
            arrived(mom_s, "mom")
        arrived(sib_g.at[0, r], "dd0", r)
        chip_terms(0, r)
        send(own_g.at[0, r, lo], p2a.at[r], "rs", "p2", r, dp=dp_xp)
        send(own_g.at[0, r, hi], m2b.at[r], "rs", "p2", r, dp=dp_xm)

    def near(r):
        arrived(sib_g.at[pl.ds(1, 3), r], "dd1", r)
        chip_terms(1, r)
        send(own_g.at[1, r, hi], p1b.at[r], "rs", "p1", r, dp=dp_xp)
        chip_terms(2, r)
        send(own_g.at[2, r, lo], m1a.at[r], "rs", "p1", r, dp=dp_xm)

    def sum_(r):
        arrived(own_g.at[0, r], "p2", r)
        own_g[1, r, lo] = own_g[1, r, lo] + p2a[r]
        send(own_g.at[1, r, lo], p1a.at[r], "rs", "p1", r, dp=dp_xp)
        own_g[2, r, hi] = own_g[2, r, hi] + m2b[r]
        send(own_g.at[2, r, hi], m1b.at[r], "rs", "p1", r, dp=dp_xm)

    started = []

    def gather1(r):
        if not started:
            sq_own[...] = jnp.zeros_like(sq_own)
        started.append(r)
        arrived(own_g.at[pl.ds(0, 2), r], "p1", r)
        chip_terms(3, r)
        for half, (near_ref, far_ref) in enumerate(((m1a, p1a), (p1b, m1b))):
            ds = pl.ds(half * 4, 4)
            total = own_g[3, r, ds] + (near_ref[r] + far_ref[r])
            mix[ds, pl.ds(r * RC, RC)] = total
            upd = ((1.0 + MOMENTUM) * total).astype(BF16)
            gath[z, y, r, ds] = upd
            upd = upd.astype(F32)
            sq_own[...] += jnp.sum((upd * upd).reshape(RC // 2, 8, 128), axis=0)
        for near_first in ((tp_zp, tp_yp), (tp_zm, tp_ym), (tp_z2, tp_y2)):
            send(gath.at[z, y, r, lo], gath.at[z, y, r, lo], "g1", "g1", r, tp=near_first[0])
            send(gath.at[z, y, r, hi], gath.at[z, y, r, hi], "g1", "g1", r, tp=near_first[1])
        for t in (tp_yp, tp_ym):
            send(gath.at[z, y, r, lo], gath.at[z, y, r, lo], "g2", "g2", r, tp=t)
        for t in (tp_zp, tp_zm):
            send(gath.at[z, y, r, hi], gath.at[z, y, r, hi], "g2", "g2", r, tp=t)
        if len(started) == NC:
            for t in (tp_zp, tp_zm, tp_z2):
                send(sq_own, sq_z.at[z], "sq", "sqz", tp=t)

    def gather2(r):
        arrived(gath.at[0, pl.ds(0, 3), r], "g1", r)
        for other in (zp, zm, z2):
            for t in (tp_yp, tp_ym):
                send(gath.at[other, y, r, lo], gath.at[other, y, r, lo], "g2", "g2", r, tp=t)
        for other in (yp, ym, y2):
            for t in (tp_zp, tp_zm):
                send(gath.at[z, other, r, hi], gath.at[z, other, r, hi], "g2", "g2", r, tp=t)

    def forward2(r):
        arrived(gath.at[pl.ds(0, 2), :, r], "g2", r)
        for block, t in ((gath.at[:, ym, r, pl.ds(0, 2)], tp_yp), (gath.at[:, yp, r, pl.ds(2, 2)], tp_ym),
                         (gath.at[zm, :, r, pl.ds(4, 2)], tp_zp), (gath.at[zp, :, r, pl.ds(6, 2)], tp_zm)):
            send(block, block, "g2", "f2", r, tp=t)

    inv = []

    def sums(_):
        sq_z[z] = sq_own[...]
        arrived(sq_z.at[pl.ds(0, 3)], "sqz")
        sq_y[y] = jnp.sum(sq_z[...], axis=0)
        for t in (tp_yp, tp_ym, tp_y2):
            send(sq_y.at[y], sq_y.at[y], "sq", "sqy", tp=t)

    def norm(_):
        arrived(sq_y.at[pl.ds(0, 3)], "sqy")
        total = jnp.sum(jnp.sum(sq_y[...], axis=0), keepdims=True)
        inv.append(1.0 / (jnp.sqrt(total) + NORM_EPS))

    def scale(r):
        arrived(gath.at[0, :, r], "f2", r)
        for i in range(4):
            for j in range(4):
                block = gath[i, j, r].reshape(CR, 128).astype(F32) * inv[0]
                x_cur[pl.ds(r * CR, CR), pl.ds(i * 512 + j * 128, 128)] = block.astype(BF16)

    def gram_rows(i):
        rows, left = pl.ds(i * 256, 256), pl.ds(0, i * 256)
        block = dot_nt(x_cur[rows, :], x_cur[pl.ds(0, i * 256 + 256), :]).astype(BF16)
        gram[rows, pl.ds(0, i * 256 + 256)] = block
        if i:
            gram[left, rows] = block[:, :i * 256].T

    def mirror_store(dst, block, first):
        dst[pl.ds(first, ROWS - first), pl.ds(first, 256)] = block
        if first + 256 < ROWS:
            dst[pl.ds(first, 256), pl.ds(first + 256, ROWS - first - 256)] = block[256:, :].T

    stages = {"dd": dd, "far": far, "near": near, "sum": sum_, "gather1": gather1, "gather2": gather2,
              "forward2": forward2, "norm": norm, "scale": scale, "sums": sums, "gram": gram_rows}
    for name, r in ORDER:
        with jax.named_scope(f"{name}_{r}"):
            stages[name](r)

    w_own = pltpu.make_async_copy(weight, w_full.at[:, me], local_sems.at[NC + 1])
    w_own.start()
    for d in (dp_xp, dp_xm, dp_x2):
        send(weight, w_full.at[:, me], "w3", "w3", dp=d)
    send(weight, w_full.at[:, me], "w4", "w4", dp=sib)

    for d in peers():
        send(mix.at[d], mom_r.at[me], "back", "back", dp=d)

    def polynomial():
        for first in range(0, ROWS, 256):
            below, cols = pl.ds(first, ROWS - first), pl.ds(first, 256)
            square = dot_nn(gram[below, :], gram[:, cols])
            mirror_store(poly, (COEF_B * gram[below, cols].astype(F32) + COEF_C * square).astype(BF16), first)

    @pl.loop(0, NS_STEPS - 1)
    def _(step):
        polynomial()
        for first in range(0, COLS, 256):
            cols = pl.ds(first, 256)
            block = x_cur[:, cols]
            prod = dot_nn(poly[...], block)
            x_cur[:, cols] = (COEF_A * block.astype(F32) + prod).astype(BF16)
        for first in range(0, ROWS, 256):
            below = pl.ds(first, ROWS - first)
            mirror_store(gram, dot_nt(x_cur[below, :], x_cur[pl.ds(first, 256), :]).astype(BF16), first)

    arrived(w_full.at[:, pl.ds(0, 3)], "w3")
    for d in (dp_xm, dp_xp, dp_x2):
        send(w_full.at[:, d], w_full.at[:, d], "w4", "w4", dp=sib)

    polynomial()
    own_cols = pl.ds(pl.multiple_of(tp * 128, 128), 128)
    block = x_cur[:, own_cols]

    def last(group, src, **device):
        send(src, src, "last", group, **device)

    final = (COEF_A * block.astype(F32) + dot_nn(poly[...], block)).astype(BF16)
    for r in range(NC):
        for d in range(8):
            x_full[me, pl.ds(d * 128 + r * RC, RC)] = final[r * CR + d * RC:r * CR + (d + 1) * RC]
    top, bot = pl.ds(0, 512), pl.ds(512, 512)
    last("fa", x_full.at[me, top], dp=dp_xp)
    last("fa", x_full.at[me, bot], dp=dp_xm)
    last("fb", x_full.at[me, bot], dp=dp_xp)
    last("fb", x_full.at[me, top], dp=dp_xm)
    last("fs", x_full.at[me], dp=sib)

    w_own.wait()
    arrived(w_full.at[:, pl.ds(0, 4)], "w4")

    def sent(*pairs):
        for group, like in pairs:
            drain(send_sems.at[SEND_GROUPS.index(group)], like)

    def finish(mat):
        lr = rate[mat]
        dec = decay[0]
        wf = w_full[mat].reshape(ROWS, 128)
        new = wf - lr * (OUT_SCALE * x_full[mat].astype(F32) + dec * wf)
        full_out[mat] = new.astype(BF16)
        wo = w_full[mat, me]
        rows = pl.ds(pl.multiple_of(me * 128, 128), 128)
        pair_out[1, mat] = wo - lr * (OUT_SCALE * x_full[mat, rows].astype(F32) + dec * wo)

    mom_r[me] = mix[me]
    arrived(mom_r.at[pl.ds(0, 7)], "back")
    pair_out[0] = mom_r[...] + (MOMENTUM - MIX) * mom_v[...]

    pair = x_full.at[0]
    finish(me)
    sent(("dd", own_g), ("rs", own_g.at[pl.ds(0, 3)]), ("mom", mom_s),
         ("back", mom_r.at[pl.ds(0, 7)]), ("sq", mom_r.at[0, pl.ds(0, 48)]), ("g1", gath.at[0, pl.ds(0, 3)]),
         ("g2", gath.at[pl.ds(0, 3)]), ("w3", w_full.at[:, pl.ds(0, 3)]), ("w4", w_full.at[:, pl.ds(0, 4)]))
    arrived(pair, "fa")
    last("q", x_full.at[dp_xm, top], dp=dp_xp)
    last("q", x_full.at[dp_xp, bot], dp=dp_xm)
    arrived(pair, "fs")
    finish(sib)
    arrived(pair, "fb")
    last("s1", x_full.at[dp_xm], dp=sib)
    last("s1", x_full.at[dp_xp], dp=sib)
    finish(dp_xm)
    finish(dp_xp)
    arrived(x_full.at[pl.ds(0, 2)], "s1")
    finish(xm * 2 + 1 - core)
    finish(xp * 2 + 1 - core)
    arrived(pair, "q")
    last("s2", x_full.at[dp_x2, top], dp=sib)
    last("s2", x_full.at[dp_x2, bot], dp=sib)
    finish(dp_x2)
    arrived(pair, "s2")
    finish(x2 * 2 + 1 - core)

    sent(("last", x_full.at[pl.ds(0, 7)]))


def solution(mesh):
    def local_step(grad_local, mom_local, weight_local, learn_rate, decay_rate):
        hbm = pl.BlockSpec(memory_space=pltpu.HBM)
        vmem = pl.BlockSpec(memory_space=pltpu.VMEM)
        smem = pl.BlockSpec(memory_space=pltpu.SMEM)
        V = pltpu.VMEM
        pair, weight_low = pl.pallas_call(
            muon_kernel,
            out_shape=(
                V((2, 8, 128, 128), F32),
                V((8, 1024, 128), BF16),
            ),
            in_specs=[hbm, hbm, hbm, smem, smem],
            out_specs=(vmem, vmem),
            scratch_shapes=[
                V((4, NC, 8, RC, 128), F32), V((4, NC, 8, RC, 128), F32),
                V((NC, 4, RC, 128), F32), V((NC, 4, RC, 128), F32), V((NC, 4, RC, 128), F32),
                V((NC, 4, RC, 128), F32), V((NC, 4, RC, 128), F32), V((NC, 4, RC, 128), F32),
                V((8, 128, 128), F32), V((4, 128, 128), F32), V((8, 128, 128), F32), V((8, 128, 128), F32),
                V((4, 4, NC, 8, RC, 128), BF16), V((8, 128), F32), V((4, 8, 128), F32), V((4, 8, 128), F32),
                V((ROWS, COLS), BF16), V((ROWS, ROWS), BF16), V((ROWS, ROWS), BF16),
                V((8, 8, 128, 128), F32), V((8, ROWS, 128), BF16),
                pltpu.SemaphoreType.DMA((len(SEND_GROUPS),)), pltpu.SemaphoreType.DMA((N_RECV,)),
                pltpu.SemaphoreType.DMA((N_LOCAL,)),
            ],
            compiler_params=pltpu.CompilerParams(
                collective_id=0, has_side_effects=True, vmem_limit_bytes=63_400_000),
            name="muon_step",
        )(grad_local.reshape(8, 8, 128, 128), mom_local, weight_local, learn_rate, decay_rate.reshape(1))
        return pair[0], pair[1], weight_low

    return jax.shard_map(
        local_step,
        mesh=mesh,
        in_specs=(P(("rep", "dp"), None, None, "tp"), P("rep", "dp", "tp"), P("rep", "dp", "tp"), P("rep"), P()),
        out_specs=(P("rep", "dp", "tp"), P("rep", "dp", "tp"), P("rep", None, "tp")),
        check_vma=False,
    )
```

```python
import math
import jax
import jax.numpy as jnp
from jax import lax
from jax.experimental import pallas as pl
from jax.experimental.pallas import tpu as pltpu
from jax.sharding import PartitionSpec as P

MOMENTUM = 0.95
NS_STEPS = 5
COEF_A = 3.4445
COEF_B = -4.7750
COEF_C = 2.0315
NORM_EPS = 1e-7
F32 = jnp.float32
BF16 = jnp.bfloat16

MATS, ROWS, COLS = 8, 1024, 2048
NC = 8
RC = 128 // NC
CR = 8 * RC
MIX = MOMENTUM * MOMENTUM / (1.0 + MOMENTUM)
OUT_SCALE = 0.2 * math.sqrt(max(ROWS, COLS))


def dot_nt(lhs, rhs):
    return lax.dot_general(lhs, rhs, (((1,), (1,)), ((), ())), preferred_element_type=F32)


def dot_nn(lhs, rhs):
    return lax.dot_general(lhs, rhs, (((1,), (0,)), ((), ())), preferred_element_type=F32)


ORDER = (
    ("dd", 0), ("dd", 4), ("dd", 6), ("far", 0), ("dd", 2), ("near", 0), ("dd", 3), ("dd", 1), ("far", 2), ("far", 1),
    ("near", 2), ("sum", 0), ("dd", 5), ("near", 1), ("far", 3), ("sum", 1), ("sum", 2), ("near", 3), ("gather1", 0),
    ("far", 4), ("dd", 7), ("sum", 3), ("far", 5), ("gather1", 1), ("near", 4), ("far", 6), ("gather1", 2),
    ("sum", 4), ("far", 7), ("gather2", 0), ("gather1", 3), ("near", 5), ("sum", 5), ("near", 7), ("gather2", 1),
    ("near", 6), ("sum", 6), ("gather2", 2), ("gather1", 4), ("sum", 7), ("forward2", 0), ("gather1", 5),
    ("gather2", 3), ("gather1", 6), ("gather1", 7), ("forward2", 1), ("gather2", 4), ("gather2", 5), ("forward2", 2),
    ("gather2", 6), ("sums", 0), ("gather2", 7), ("forward2", 3), ("forward2", 4), ("forward2", 5), ("forward2", 6),
    ("forward2", 7), ("norm", 0), ("scale", 2), ("scale", 1), ("scale", 0), ("scale", 3), ("gram", 0), ("gram", 1),
    ("scale", 4), ("scale", 5), ("gram", 2), ("scale", 6), ("scale", 7), ("gram", 3),
)

CHUNK_GROUPS = ("dd0", "dd1", "p2", "p1", "g1", "g2", "f2")
LATE_GROUPS = ("mom", "sqz", "sqy", "back", "w3", "w4", "fa", "fb", "fs", "s1", "q", "s2")
SEND_GROUPS = ("dd", "rs", "mom", "back", "sq", "g1", "g2", "w3", "w4", "last")
N_RECV = NC * len(CHUNK_GROUPS) + len(LATE_GROUPS)
N_LOCAL = 4


def muon_kernel(grad, mom, weight, rate, decay, pair_out, full_out,
                own_g, sib_g, p2a, p1b, p1a, m2b, m1a, m1b, mom_v, mom_s, mix, mom_r, gath, sq_own, sq_z, sq_y,
                x_cur, gram, poly, w_full, x_full, send_sems, recv_sems, local_sems):
    me = lax.axis_index("dp")
    tp = lax.axis_index("tp")
    x, core = lax.div(me, 2), lax.rem(me, 2)
    z, y = lax.div(tp, 4), lax.rem(tp, 4)
    xp, xm, x2 = lax.rem(x + 1, 4), lax.rem(x + 3, 4), lax.rem(x + 2, 4)
    yp, ym, y2 = lax.rem(y + 1, 4), lax.rem(y + 3, 4), lax.rem(y + 2, 4)
    zp, zm, z2 = lax.rem(z + 1, 4), lax.rem(z + 3, 4), lax.rem(z + 2, 4)
    sib = x * 2 + 1 - core
    dp_xp, dp_xm, dp_x2 = xp * 2 + core, xm * 2 + core, x2 * 2 + core
    tp_yp, tp_ym, tp_y2 = z * 4 + yp, z * 4 + ym, z * 4 + y2
    tp_zp, tp_zm, tp_z2 = zp * 4 + y, zm * 4 + y, z2 * 4 + y
    slots = (x2, xp, xm, x)

    def recv_sem(group, r=None):
        if r is None:
            return recv_sems.at[NC * len(CHUNK_GROUPS) + LATE_GROUPS.index(group)]
        return recv_sems.at[r * len(CHUNK_GROUPS) + CHUNK_GROUPS.index(group)]

    def send(src, dst, sent, group, r=None, **device):
        pltpu.make_async_remote_copy(
            src_ref=src, dst_ref=dst, send_sem=send_sems.at[SEND_GROUPS.index(sent)], recv_sem=recv_sem(group, r),
            device_id=device, device_id_type=pl.DeviceIdType.MESH,
        ).start()

    def drain(sem, like):
        pltpu.make_async_copy(like, like, sem).wait()

    def arrived(like, group, r=None):
        drain(recv_sem(group, r), like)

    def peers(rest=7):
        return [lax.rem(me + i, 8) for i in range(1, rest + 1)]

    barrier = pltpu.get_barrier_semaphore()
    for d in peers():
        pl.semaphore_signal(barrier, inc=1, device_id={"dp": d}, device_id_type=pl.DeviceIdType.MESH)
    for t in (tp_yp, tp_ym, tp_y2, tp_zp, tp_zm, tp_z2):
        pl.semaphore_signal(barrier, inc=1, device_id={"tp": t}, device_id_type=pl.DeviceIdType.MESH)
    for r in range(NC):
        for s in range(4):
            pltpu.make_async_copy(grad.at[slots[s] * 2 + core, :, pl.ds(r * RC, RC), :], own_g.at[s, r],
                                  local_sems.at[min(r, 1)]).start()
    mom_load = pltpu.make_async_copy(mom, mom_v, local_sems.at[2])
    mom_load.start()

    with jax.named_scope("entry"):
        pl.semaphore_wait(barrier, 13)

    def dd(r):
        for s in range(4):
            send(grad.at[slots[s] * 2 + 1 - core, :, pl.ds(r * RC, RC), :], sib_g.at[s, r], "dd", "dd1" if s else "dd0",
                 r, dp=sib)
        if r == 0:
            for s in range(4):
                send(mom.at[slots[s] * 2 + 1 - core], mom_s.at[s], "mom", "mom", dp=sib)

    lo, hi = pl.ds(0, 4), pl.ds(4, 4)

    def chip_terms(s, r):
        rows = pl.ds(r * RC, RC)
        own_g[s, r] = (own_g[s, r] + sib_g[s, r]) * (1.0 / 8.0)
        own_g[s, r, me] = own_g[s, r, me] + MIX * mom_v[slots[s] * 2 + core, rows]
        own_g[s, r, sib] = own_g[s, r, sib] + MIX * mom_s[s, rows]

    loaded = []

    def far(r):
        if r == 0:
            drain(local_sems.at[0], own_g.at[:, 0])
        elif not loaded:
            drain(local_sems.at[1], own_g.at[:, pl.ds(1, NC - 1)])
            loaded.append(r)
        if r == 0:
            mom_load.wait()
            arrived(mom_s, "mom")
        arrived(sib_g.at[0, r], "dd0", r)
        chip_terms(0, r)
        send(own_g.at[0, r, lo], p2a.at[r], "rs", "p2", r, dp=dp_xp)
        send(own_g.at[0, r, hi], m2b.at[r], "rs", "p2", r, dp=dp_xm)

    def near(r):
        arrived(sib_g.at[pl.ds(1, 3), r], "dd1", r)
        chip_terms(1, r)
        send(own_g.at[1, r, hi], p1b.at[r], "rs", "p1", r, dp=dp_xp)
        chip_terms(2, r)
        send(own_g.at[2, r, lo], m1a.at[r], "rs", "p1", r, dp=dp_xm)

    def sum_(r):
        arrived(own_g.at[0, r], "p2", r)
        own_g[1, r, lo] = own_g[1, r, lo] + p2a[r]
        send(own_g.at[1, r, lo], p1a.at[r], "rs", "p1", r, dp=dp_xp)
        own_g[2, r, hi] = own_g[2, r, hi] + m2b[r]
        send(own_g.at[2, r, hi], m1b.at[r], "rs", "p1", r, dp=dp_xm)

    started = []

    def gather1(r):
        if not started:
            sq_own[...] = jnp.zeros_like(sq_own)
        started.append(r)
        arrived(own_g.at[pl.ds(0, 2), r], "p1", r)
        chip_terms(3, r)
        for half, (near_ref, far_ref) in enumerate(((m1a, p1a), (p1b, m1b))):
            ds = pl.ds(half * 4, 4)
            total = own_g[3, r, ds] + (near_ref[r] + far_ref[r])
            mix[ds, pl.ds(r * RC, RC)] = total
            upd = ((1.0 + MOMENTUM) * total).astype(BF16)
            gath[z, y, r, ds] = upd
            upd = upd.astype(F32)
            sq_own[...] += jnp.sum((upd * upd).reshape(RC // 2, 8, 128), axis=0)
        for near_first in ((tp_zp, tp_yp), (tp_zm, tp_ym), (tp_z2, tp_y2)):
            send(gath.at[z, y, r, lo], gath.at[z, y, r, lo], "g1", "g1", r, tp=near_first[0])
            send(gath.at[z, y, r, hi], gath.at[z, y, r, hi], "g1", "g1", r, tp=near_first[1])
        for t in (tp_yp, tp_ym):
            send(gath.at[z, y, r, lo], gath.at[z, y, r, lo], "g2", "g2", r, tp=t)
        for t in (tp_zp, tp_zm):
            send(gath.at[z, y, r, hi], gath.at[z, y, r, hi], "g2", "g2", r, tp=t)
        if len(started) == NC:
            for t in (tp_zp, tp_zm, tp_z2):
                send(sq_own, sq_z.at[z], "sq", "sqz", tp=t)

    def gather2(r):
        arrived(gath.at[0, pl.ds(0, 3), r], "g1", r)
        for other in (zp, zm, z2):
            for t in (tp_yp, tp_ym):
                send(gath.at[other, y, r, lo], gath.at[other, y, r, lo], "g2", "g2", r, tp=t)
        for other in (yp, ym, y2):
            for t in (tp_zp, tp_zm):
                send(gath.at[z, other, r, hi], gath.at[z, other, r, hi], "g2", "g2", r, tp=t)

    def forward2(r):
        arrived(gath.at[pl.ds(0, 2), :, r], "g2", r)
        for block, t in ((gath.at[:, ym, r, pl.ds(0, 2)], tp_yp), (gath.at[:, yp, r, pl.ds(2, 2)], tp_ym),
                         (gath.at[zm, :, r, pl.ds(4, 2)], tp_zp), (gath.at[zp, :, r, pl.ds(6, 2)], tp_zm)):
            send(block, block, "g2", "f2", r, tp=t)

    inv = []

    def sums(_):
        sq_z[z] = sq_own[...]
        arrived(sq_z.at[pl.ds(0, 3)], "sqz")
        sq_y[y] = jnp.sum(sq_z[...], axis=0)
        for t in (tp_yp, tp_ym, tp_y2):
            send(sq_y.at[y], sq_y.at[y], "sq", "sqy", tp=t)

    def norm(_):
        arrived(sq_y.at[pl.ds(0, 3)], "sqy")
        total = jnp.sum(jnp.sum(sq_y[...], axis=0), keepdims=True)
        inv.append(1.0 / (jnp.sqrt(total) + NORM_EPS))

    def scale(r):
        arrived(gath.at[0, :, r], "f2", r)
        for i in range(4):
            for j in range(4):
                block = gath[i, j, r].reshape(CR, 128).astype(F32) * inv[0]
                x_cur[pl.ds(r * CR, CR), pl.ds(i * 512 + j * 128, 128)] = block.astype(BF16)

    def gram_rows(i):
        rows, left = pl.ds(i * 256, 256), pl.ds(0, i * 256)
        block = dot_nt(x_cur[rows, :], x_cur[pl.ds(0, i * 256 + 256), :]).astype(BF16)
        gram[rows, pl.ds(0, i * 256 + 256)] = block
        if i:
            gram[left, rows] = block[:, :i * 256].T

    def mirror_store(dst, block, first):
        dst[pl.ds(first, ROWS - first), pl.ds(first, 256)] = block
        if first + 256 < ROWS:
            dst[pl.ds(first, 256), pl.ds(first + 256, ROWS - first - 256)] = block[256:, :].T

    stages = {"dd": dd, "far": far, "near": near, "sum": sum_, "gather1": gather1, "gather2": gather2,
              "forward2": forward2, "norm": norm, "scale": scale, "sums": sums, "gram": gram_rows}
    for name, r in ORDER:
        with jax.named_scope(f"{name}_{r}"):
            stages[name](r)

    w_own = pltpu.make_async_copy(weight, w_full.at[:, me], local_sems.at[3])
    w_own.start()
    for d in (dp_xp, dp_xm, dp_x2):
        send(weight, w_full.at[:, me], "w3", "w3", dp=d)
    send(weight, w_full.at[:, me], "w4", "w4", dp=sib)

    for d in peers():
        send(mix.at[d], mom_r.at[me], "back", "back", dp=d)

    def polynomial():
        for first in range(0, ROWS, 256):
            below, cols = pl.ds(first, ROWS - first), pl.ds(first, 256)
            square = dot_nn(gram[below, :], gram[:, cols])
            mirror_store(poly, (COEF_B * gram[below, cols].astype(F32) + COEF_C * square).astype(BF16), first)

    @pl.loop(0, NS_STEPS - 1)
    def _(step):
        polynomial()
        for first in range(0, COLS, 256):
            cols = pl.ds(first, 256)
            block = x_cur[:, cols]
            prod = dot_nn(poly[...], block)
            x_cur[:, cols] = (COEF_A * block.astype(F32) + prod).astype(BF16)
        for first in range(0, ROWS, 256):
            below = pl.ds(first, ROWS - first)
            mirror_store(gram, dot_nt(x_cur[below, :], x_cur[pl.ds(first, 256), :]).astype(BF16), first)

    arrived(w_full.at[:, pl.ds(0, 3)], "w3")
    for d in (dp_xm, dp_xp, dp_x2):
        send(w_full.at[:, d], w_full.at[:, d], "w4", "w4", dp=sib)

    polynomial()
    own_cols = pl.ds(pl.multiple_of(tp * 128, 128), 128)
    block = x_cur[:, own_cols]

    def last(group, src, **device):
        send(src, src, "last", group, **device)

    final = (COEF_A * block.astype(F32) + dot_nn(poly[...], block)).astype(BF16)
    for r in range(NC):
        for d in range(8):
            x_full[me, pl.ds(d * 128 + r * RC, RC)] = final[r * CR + d * RC:r * CR + (d + 1) * RC]
    top, bot = pl.ds(0, 512), pl.ds(512, 512)
    last("fa", x_full.at[me, top], dp=dp_xp)
    last("fa", x_full.at[me, bot], dp=dp_xm)
    last("fb", x_full.at[me, bot], dp=dp_xp)
    last("fb", x_full.at[me, top], dp=dp_xm)
    last("fs", x_full.at[me], dp=sib)

    w_own.wait()
    arrived(w_full.at[:, pl.ds(0, 4)], "w4")

    def sent(*pairs):
        for group, like in pairs:
            drain(send_sems.at[SEND_GROUPS.index(group)], like)

    def finish(mat):
        lr = rate[mat]
        dec = decay[0]
        wf = w_full[mat].reshape(ROWS, 128)
        new = wf - lr * (OUT_SCALE * x_full[mat].astype(F32) + dec * wf)
        full_out[mat] = new.astype(BF16)
        wo = w_full[mat, me]
        rows = pl.ds(pl.multiple_of(me * 128, 128), 128)
        pair_out[1, mat] = wo - lr * (OUT_SCALE * x_full[mat, rows].astype(F32) + dec * wo)

    mom_r[me] = mix[me]
    arrived(mom_r.at[pl.ds(0, 7)], "back")
    pair_out[0] = mom_r[...] + (MOMENTUM - MIX) * mom_v[...]

    pair = x_full.at[0]
    finish(me)
    sent(("dd", own_g), ("rs", own_g.at[pl.ds(0, 3)]), ("mom", mom_s),
         ("back", mom_r.at[pl.ds(0, 7)]), ("sq", mom_r.at[0, pl.ds(0, 48)]), ("g1", gath.at[0, pl.ds(0, 3)]),
         ("g2", gath.at[pl.ds(0, 3)]), ("w3", w_full.at[:, pl.ds(0, 3)]), ("w4", w_full.at[:, pl.ds(0, 4)]))
    arrived(pair, "fa")
    last("q", x_full.at[dp_xm, top], dp=dp_xp)
    last("q", x_full.at[dp_xp, bot], dp=dp_xm)
    arrived(pair, "fs")
    finish(sib)
    arrived(pair, "fb")
    last("s1", x_full.at[dp_xm], dp=sib)
    last("s1", x_full.at[dp_xp], dp=sib)
    finish(dp_xm)
    finish(dp_xp)
    arrived(x_full.at[pl.ds(0, 2)], "s1")
    finish(xm * 2 + 1 - core)
    finish(xp * 2 + 1 - core)
    arrived(pair, "q")
    last("s2", x_full.at[dp_x2, top], dp=sib)
    last("s2", x_full.at[dp_x2, bot], dp=sib)
    finish(dp_x2)
    arrived(pair, "s2")
    finish(x2 * 2 + 1 - core)

    sent(("last", x_full.at[pl.ds(0, 7)]))


def solution(mesh):
    def local_step(grad_local, mom_local, weight_local, learn_rate, decay_rate):
        hbm = pl.BlockSpec(memory_space=pltpu.HBM)
        vmem = pl.BlockSpec(memory_space=pltpu.VMEM)
        smem = pl.BlockSpec(memory_space=pltpu.SMEM)
        V = pltpu.VMEM
        pair, weight_low = pl.pallas_call(
            muon_kernel,
            out_shape=(
                V((2, 8, 128, 128), F32),
                V((8, 1024, 128), BF16),
            ),
            in_specs=[hbm, hbm, hbm, smem, smem],
            out_specs=(vmem, vmem),
            scratch_shapes=[
                V((4, NC, 8, RC, 128), F32), V((4, NC, 8, RC, 128), F32),
                V((NC, 4, RC, 128), F32), V((NC, 4, RC, 128), F32), V((NC, 4, RC, 128), F32),
                V((NC, 4, RC, 128), F32), V((NC, 4, RC, 128), F32), V((NC, 4, RC, 128), F32),
                V((8, 128, 128), F32), V((4, 128, 128), F32), V((8, 128, 128), F32), V((8, 128, 128), F32),
                V((4, 4, NC, 8, RC, 128), BF16), V((8, 128), F32), V((4, 8, 128), F32), V((4, 8, 128), F32),
                V((ROWS, COLS), BF16), V((ROWS, ROWS), BF16), V((ROWS, ROWS), BF16),
                V((8, 8, 128, 128), F32), V((8, ROWS, 128), BF16),
                pltpu.SemaphoreType.DMA((len(SEND_GROUPS),)), pltpu.SemaphoreType.DMA((N_RECV,)),
                pltpu.SemaphoreType.DMA((N_LOCAL,)),
            ],
            compiler_params=pltpu.CompilerParams(
                collective_id=0, has_side_effects=True, vmem_limit_bytes=63_400_000),
            name="muon_step",
        )(grad_local.reshape(8, 8, 128, 128), mom_local, weight_local, learn_rate, decay_rate.reshape(1))
        return pair[0], pair[1], weight_low

    return jax.shard_map(
        local_step,
        mesh=mesh,
        in_specs=(P(("rep", "dp"), None, None, "tp"), P("rep", "dp", "tp"), P("rep", "dp", "tp"), P("rep"), P()),
        out_specs=(P("rep", "dp", "tp"), P("rep", "dp", "tp"), P("rep", None, "tp")),
        check_vma=False,
    )
```
